32 devices in a mesh: grp: 4 (over x, core), seq: 8 (over z, y).
Axes of the slice: x: 2, y: 2, z: 4, core: 2. Of those that a mesh axis runs over, the one named last changes fastest.
Arguments:
- patches: bfloat16 [2048, 1280], P(('grp', 'seq')), may hold values from -60 to 60
- piece_ids: int32 [32, 64], P(('grp', 'seq')), may hold values from 0 to 2, never falling along the last dimension, each value on 1 to 48 neighbouring positions
- vit_gain: float32 [1280], replicated, may hold values from 0.25 to 1.75
- vit_qkv: bfloat16 [1280, 3840], replicated
- vit_out: bfloat16 [1280, 1280], replicated, may hold values from -0.15625 to 0.15625
- merge_gain: float32 [1280], replicated, may hold values from 0.25 to 1.75
- merge_up: bfloat16 [5120, 5120], P(None, 'seq'), may hold values from -0.078125 to 0.078125
- merge_down: bfloat16 [5120, 8192], P(None, 'seq'), may hold values from -0.078125 to 0.078125
- dest: int32 [512], P(('grp', 'seq')), may hold values from 0 to 7, as said below
- tokens: bfloat16 [8192, 8192], P(('grp', 'seq')), may hold values from -60 to 60
- image_index: int32 [8192], P(('grp', 'seq')), may hold values from 0 to 32, as said below
- doc_lengths: int32 [4, 4], P('grp'), may hold values from 1 to 1024, 2048 in all within a row
- attn_gain: float32 [8192], replicated, may hold values from 0.25 to 1.75
- attn_qkv: bfloat16 [8192, 768], P(('grp', 'seq'))
- attn_out: bfloat16 [512, 8192], P(None, ('grp', 'seq')), may hold values from -0.25 to 0.25
Outputs:
- layer_out: bfloat16 [8192, 8192], P(('grp', 'seq'))
The draws below stay inside these ranges and needn't reach their ends.
Inputs may be any that keep to these rules, and one draw needn't show every extreme that they name: `dest`: within each aligned block of 16 rows (one device's merged rows), exactly 4 distinct values occur, each exactly 4 times, and in every group one device is named by every device of the group. `image_index`: 32 marks a text token. A value k < 32 on a device names the merged row that the device of seq index k // 4 in its group sends to it as its (k % 4)-th row in row order; each such row is named by exactly one token of the receiving device, and no other values occur. `piece_ids`: piece numbers never fall within a window. `doc_lengths`: each group's documents fill its 2048 positions.
All inputs are finite; a program needn't handle non-finite values.
Results may differ from the reference program's by a relative error of at most 0.0093.
The reference program's roundings to bfloat16 on the way count: a program that leaves them out, or rounds other values in their place, can miss the bound.
Values may be sent and summed in bfloat16 or wider, within the bound.
A program may use at most 192 MiB of HBM per device.

```python
import math
import jax
import jax.numpy as jnp
import numpy as np
from jax import lax

D = 8192
VD = 1280
VHEADS = 16
HEAD = 128
HQ = 4
WIN = 64
DOCS = 4
TOK_DEV = 256
M_DEV = 16
CAP = 4
SLOTS = 32
PATCHES = 2048
WINDOWS = 32
MERGED = 512
GROUP_TOK = 2048
TOKENS = 8192
MOST_DOC = 1024
N_GRP = 4
N_SEQ = 8


def scaled_field(key, row_count, col_count):
    parts = jax.random.split(key, 3)
    row_scale = jnp.exp(jax.random.uniform(parts[1], (row_count, 1), jnp.float32, jnp.log(0.3), jnp.log(3.0)))
    col_scale = jnp.exp(jax.random.uniform(parts[2], (1, col_count), jnp.float32, jnp.log(0.3), jnp.log(3.0)))
    base = jnp.clip(jax.random.normal(parts[0], (row_count, col_count), jnp.float32), -6.0, 6.0)
    return base * row_scale * col_scale


def draw_patches(key, part):
    return scaled_field(jax.random.fold_in(key, 11), PATCHES, VD).astype(jnp.bfloat16)


def draw_tokens(key, part):
    return scaled_field(jax.random.fold_in(key, 12), TOKENS, D).astype(jnp.bfloat16)


def draw_vit_qkv(key, part):
    parts = jax.random.split(jax.random.fold_in(key, 13), 1)
    base = jnp.clip(jax.random.normal(parts[0], (VD, 3 * VD), jnp.float32), -6.0, 6.0) * VD ** (-0.5)
    return base.astype(jnp.bfloat16)


def draw_attn_qkv(key, part):
    parts = jax.random.split(jax.random.fold_in(key, 14), 1)
    base = jnp.clip(jax.random.normal(parts[0], (D, (HQ + 2) * HEAD), jnp.float32), -6.0, 6.0) * D ** (-0.5)
    return base.astype(jnp.bfloat16)


def route_tables(key):
    base_key = jax.random.fold_in(key, 5)
    fanout = N_SEQ // 2
    sequence_ids = jnp.arange(N_SEQ, dtype=jnp.int32)
    row_ids = jnp.arange(M_DEV, dtype=jnp.int32)
    slot_ids = jnp.arange(CAP, dtype=jnp.int32)

    def one_group(group_key):
        parts = jax.random.split(group_key, 4)
        preference_boost = jax.random.permutation(parts[0], N_SEQ).astype(jnp.int32)
        random_jitter = jax.random.randint(parts[1], (N_SEQ, N_SEQ), 0, 1 << 20, dtype=jnp.int32)
        extra_reward = jnp.where(preference_boost == 0, 1 << 22, (N_SEQ - preference_boost) * (1 << 14)).astype(jnp.int32)
        score_value = (random_jitter + extra_reward[None, :]) * N_SEQ + sequence_ids[None, :]
        chosen = lax.top_k(score_value, fanout)[1].astype(jnp.int32)
        shuffles = jax.vmap(lambda shuffle_key: jax.random.permutation(shuffle_key, M_DEV))(jax.random.split(parts[2], N_SEQ)).astype(jnp.int32)
        targets = jnp.take_along_axis(chosen, shuffles // CAP, axis=1)
        same = targets[:, :, None] == targets[:, None, :]
        earlier = row_ids[None, :] < row_ids[:, None]
        order = jnp.sum(same & earlier[None], axis=-1).astype(jnp.int32)
        match = (targets[None, :, None, :] == sequence_ids[:, None, None, None]) & (order[None, :, None, :] == slot_ids[None, None, :, None])
        filled = jnp.any(match, axis=-1).reshape(N_SEQ, SLOTS)
        places = jax.vmap(lambda place_key: jax.random.permutation(place_key, TOK_DEV)[:SLOTS])(jax.random.split(parts[3], N_SEQ)).astype(jnp.int32)
        token_ids = jnp.arange(TOK_DEV, dtype=jnp.int32)
        hit = (places[:, :, None] == token_ids[None, None, :]) & filled[:, :, None]
        slot_all = jnp.arange(SLOTS, dtype=jnp.int32)
        named = jnp.sum(jnp.where(hit, slot_all[None, :, None], 0), axis=1)
        index = named + jnp.where(jnp.any(hit, axis=1), 0, SLOTS)
        return (targets.reshape(-1), index.reshape(-1))
    targets_all, index_all = jax.vmap(one_group)(jax.random.split(base_key, N_GRP))
    return (targets_all.reshape(-1).astype(jnp.int32), index_all.reshape(-1).astype(jnp.int32))


def draw_dest(key, part):
    return route_tables(key)[0]


def draw_image_index(key, part):
    return route_tables(key)[1]


def block_scale(own_key, shape, pieces, low, top_value):
    loudness, own = 1.0, jax.random.fold_in(own_key, 6)
    for position, blocks in pieces:
        steps = jnp.exp(jax.random.uniform(jax.random.fold_in(own, position), (blocks,), jnp.float32, low / len(pieces), top_value / len(pieces)))
        loudness = loudness * jnp.repeat(steps, shape[position] // blocks).reshape([-1 if axis == position else 1 for axis in range(len(shape))])
    return loudness


def length_profile(count, total, bound, skew):
    weights = [(1 << 20) // math.isqrt(standing ** skew) + 1 for standing in range(2, count + 1)]
    surplus, holding = total - bound - (count - 1), [1] * (count - 1)
    while surplus > 0:
        candidates = [i for i in range(count - 1) if holding[i] < bound]
        pool, budget = sum([weights[i] for i in candidates]), surplus
        for i in candidates:
            addition = min(bound - holding[i], max(1, budget * weights[i] // pool), surplus)
            holding[i] = holding[i] + addition
            surplus = surplus - addition
    return np.array([bound] + holding)


def ragged_sizes(key, number_of, total, limit, lean):
    if number_of == 2:
        one = jax.random.randint(key, (), max(1, total - limit), min(limit, total - 1) + 1)
        return jnp.stack([one, total - one])
    sizes = jnp.asarray(length_profile(number_of, total, limit, lean), jnp.int32)
    couples = (number_of - 1) // 2
    giver, taker = sizes[1:1 + 2 * couples:2], sizes[2:2 + 2 * couples:2]
    room = jnp.minimum(giver - 1, limit - taker)
    shifted = jax.random.randint(jax.random.fold_in(key, 1), (couples,), 0, 1 << 20) % (room + 1)
    sizes = sizes.at[1:1 + 2 * couples:2].set(giver - shifted).at[2:2 + 2 * couples:2].set(taker + shifted)
    return sizes[jax.random.permutation(jax.random.fold_in(key, 2), number_of)]


def centred(own_key, shape, width, reach, cuts=(), held_as=jnp.bfloat16):
    level = block_scale(own_key, shape, cuts, -0.22, 0.18) if cuts else 1.0
    result = jax.random.normal(own_key, shape, jnp.float32) * width * level
    return jnp.minimum(jnp.maximum(result, -reach), reach).astype(held_as)


def setup_inputs(seed: int = 0) -> dict:
    key_list = jax.random.split(jax.random.key(seed), 16)
    patches = draw_patches(jax.random.fold_in(key_list[15], 71), 0)
    piece_ids = jax.vmap(lambda own: jnp.searchsorted(jnp.cumsum(ragged_sizes(own, 3, WIN, 48, 2)), jnp.arange(WIN), side="right"))(jax.random.split(key_list[1], WINDOWS)).reshape((WINDOWS, WIN)).astype(jnp.int32)
    vit_gain = jnp.clip(1.0 + 0.15 * jax.random.normal(key_list[2], (VD,), jnp.float32), 0.25, 1.75)
    vit_qkv = draw_vit_qkv(jax.random.fold_in(key_list[15], 71), 0)
    vit_out = centred(key_list[4], (VD, VD), VD ** -0.5, 0.15625)
    merge_gain = jnp.clip(1.0 + 0.15 * jax.random.normal(key_list[5], (VD,), jnp.float32), 0.25, 1.75)
    merge_up = centred(key_list[6], (4 * VD, 4 * VD), (4 * VD) ** -0.5, 0.078125, ((1, 8),))
    merge_down = centred(key_list[7], (4 * VD, D), (4 * VD) ** -0.5, 0.078125, ((1, 8),))
    dest = draw_dest(jax.random.fold_in(key_list[15], 71), 0)
    tokens = draw_tokens(jax.random.fold_in(key_list[15], 71), 0)
    image_index = draw_image_index(jax.random.fold_in(key_list[15], 71), 0)
    doc_lengths = jax.vmap(lambda own: ragged_sizes(own, DOCS, GROUP_TOK, MOST_DOC, 2))(jax.random.split(key_list[11], N_GRP)).reshape((N_GRP, DOCS)).astype(jnp.int32)
    attn_gain = jnp.clip(1.0 + 0.15 * jax.random.normal(key_list[12], (D,), jnp.float32), 0.25, 1.75)
    attn_qkv = draw_attn_qkv(jax.random.fold_in(key_list[15], 71), 0)
    attn_out = centred(key_list[14], (HQ * HEAD, D), (HQ * HEAD) ** -0.5, 0.25, ((1, 32),))
    return dict(patches=patches, piece_ids=piece_ids, vit_gain=vit_gain, vit_qkv=vit_qkv, vit_out=vit_out, merge_gain=merge_gain, merge_up=merge_up, merge_down=merge_down, dest=dest, tokens=tokens, image_index=image_index, doc_lengths=doc_lengths, attn_gain=attn_gain, attn_qkv=attn_qkv, attn_out=attn_out)


EPSILON = 1e-06

def rms_scale(inputs, gain):
    mean_square = lax.optimization_barrier(jnp.mean(inputs * inputs, axis=-1, keepdims=True))
    return inputs * lax.rsqrt(mean_square + EPSILON) * gain

def softmax_mix(scores, allowed, value_collection, spec):
    scores = jnp.where(allowed[None], scores, -1e+30)
    highest = lax.optimization_barrier(jnp.max(scores, axis=-1, keepdims=True))
    weights = jnp.exp(scores - highest)
    totals = lax.optimization_barrier(jnp.sum(weights, axis=-1))
    rounded_values = lax.optimization_barrier(weights.astype(jnp.bfloat16)).astype(jnp.float32)
    mixture = jnp.einsum(spec, rounded_values, value_collection.astype(jnp.float32))
    return mixture / jnp.transpose(totals)[:, :, None]

def window_layer(patch_rows, piece_rows, vit_gain, vit_qkv, vit_out, merge_gain):
    row_count, features = patch_rows.shape
    head_dim = features // VHEADS
    residual = patch_rows.astype(jnp.float32)
    normed = rms_scale(residual, vit_gain).astype(jnp.bfloat16)
    projected = jnp.dot(normed, vit_qkv, preferred_element_type=jnp.float32).astype(jnp.bfloat16)
    queries = projected[:, :features].reshape(row_count, VHEADS, head_dim)
    key_set = projected[:, features:2 * features].reshape(row_count, VHEADS, head_dim)
    value_collection = projected[:, 2 * features:].reshape(row_count, VHEADS, head_dim)
    scores = jnp.einsum('qhd,khd->hqk', queries.astype(jnp.float32), key_set.astype(jnp.float32)) * head_dim ** (-0.5)
    frames = jnp.arange(row_count, dtype=jnp.int32) // WIN
    allowed = (frames[:, None] == frames[None, :]) & (piece_rows[:, None] == piece_rows[None, :])
    mixture = softmax_mix(scores, allowed, value_collection, 'hqk,khd->qhd')
    mixture = mixture.reshape(row_count, features).astype(jnp.bfloat16)
    residual = residual + jnp.dot(mixture, vit_out, preferred_element_type=jnp.float32)
    merge_input = rms_scale(residual, merge_gain).astype(jnp.bfloat16)
    return merge_input.reshape(row_count // 4, 4 * features)

def attend(query_rows, query_pos, query_start, key_value, key_pos):
    row_count = query_rows.shape[0]
    head_dim = key_value.shape[1] // 2
    heads = query_rows.shape[1] // head_dim
    queries = query_rows.reshape(row_count, heads, head_dim)
    scores = jnp.einsum('qhd,kd->hqk', queries.astype(jnp.float32), key_value[:, :head_dim].astype(jnp.float32)) * head_dim ** (-0.5)
    allowed = (key_pos[None, :] >= query_start[:, None]) & (key_pos[None, :] <= query_pos[:, None])
    mixture = softmax_mix(scores, allowed, key_value[:, head_dim:], 'hqk,kd->qhd')
    return mixture.reshape(row_count, heads * head_dim).astype(jnp.bfloat16)

def slot_numbers(targets):
    row_count = targets.shape[-1]
    order = jnp.arange(row_count, dtype=jnp.int32)
    same = targets[..., :, None] == targets[..., None, :]
    earlier = order[None, :] < order[:, None]
    return lax.optimization_barrier(jnp.sum(same & earlier, axis=-1)).astype(jnp.int32)

def prefill_group(layer_in, lengths, attn_gain, attn_qkv, attn_out):
    normed = rms_scale(layer_in.astype(jnp.float32), attn_gain).astype(jnp.bfloat16)
    projected = jnp.dot(normed, attn_qkv, preferred_element_type=jnp.float32).astype(jnp.bfloat16)
    query_width = HQ * HEAD
    queries = projected[:, :query_width]
    key_value = projected[:, query_width:]
    positions = jnp.arange(GROUP_TOK, dtype=jnp.int32)
    starts = (jnp.cumsum(lengths) - lengths).astype(jnp.int32)
    doc_start = lax.optimization_barrier(jnp.max(jnp.where(starts[None, :] <= positions[:, None], starts[None, :], 0), axis=1)).astype(jnp.int32)
    block_rows = min(GROUP_TOK, 512)
    attended = lax.map(lambda parts: attend(parts[0], parts[1], parts[2], key_value, positions), (queries.reshape(-1, block_rows, query_width), positions.reshape(-1, block_rows), doc_start.reshape(-1, block_rows))).reshape(GROUP_TOK, query_width)
    update = jnp.dot(attended, attn_out, preferred_element_type=jnp.float32)
    return (layer_in.astype(jnp.float32) + update).astype(jnp.bfloat16)

def reference(patches, piece_ids, vit_gain, vit_qkv, vit_out, merge_gain, merge_up, merge_down, dest, tokens, image_index, doc_lengths, attn_gain, attn_qkv, attn_out):
    block_len = WIN
    patch_blocks = patches.reshape(PATCHES // block_len, block_len, VD)
    piece_blocks = piece_ids.reshape(PATCHES // block_len, block_len)
    merge_input = lax.map(lambda parts: window_layer(parts[0], parts[1], vit_gain, vit_qkv, vit_out, merge_gain), (patch_blocks, piece_blocks)).reshape(MERGED, 4 * VD)
    hidden = jax.nn.gelu(jnp.dot(merge_input, merge_up, preferred_element_type=jnp.float32), approximate=False).astype(jnp.bfloat16)
    merged_rows = jnp.dot(hidden, merge_down, preferred_element_type=jnp.float32).astype(jnp.bfloat16)
    merged_rows = merged_rows.reshape(N_GRP, N_SEQ, M_DEV, D)
    targets = dest.reshape(N_GRP, N_SEQ, M_DEV)
    orders = slot_numbers(targets)
    receivers = jnp.arange(N_SEQ, dtype=jnp.int32)
    row_ids = jnp.arange(M_DEV, dtype=jnp.int32)
    slot_ids = jnp.arange(CAP, dtype=jnp.int32)
    index_all = image_index.reshape(N_GRP, N_SEQ, TOK_DEV)
    token_all = tokens.reshape(N_GRP, N_SEQ, TOK_DEV, D)
    results = []
    for group in range(N_GRP):
        match = (targets[group][None, :, None, :] == receivers[:, None, None, None]) & (orders[group][None, :, None, :] == slot_ids[None, None, :, None])
        row_pick = lax.optimization_barrier(jnp.sum(jnp.where(match, row_ids, 0), axis=-1)).astype(jnp.int32)
        source_list = jnp.broadcast_to(receivers[None, :, None], row_pick.shape)
        table = merged_rows[group][source_list, row_pick].reshape(N_SEQ, SLOTS, D)
        index_rows = index_all[group]
        picked = jax.vmap(lambda table_rows, wanted: table_rows[jnp.minimum(wanted, SLOTS - 1)])(table, index_rows)
        layer_in = jnp.where((index_rows < SLOTS)[:, :, None], picked, token_all[group]).reshape(GROUP_TOK, D)
        results.append(prefill_group(layer_in, doc_lengths[group], attn_gain, attn_qkv, attn_out))
    return jnp.concatenate(results, axis=0)
```

```python
import functools
import math

import jax
import jax.numpy as jnp
from jax import lax
from jax.experimental import pallas as pl
from jax.experimental.pallas import tpu as pltpu
from jax.sharding import PartitionSpec as P

VHEADS = 16
WIN = 64
LANES = 128
EPSILON = 1e-06
AHEAD = 4
MESH = pl.DeviceIdType.MESH


def rms_scale(inputs, gain):
    mean_square = jnp.mean(inputs * inputs, axis=-1, keepdims=True)
    return inputs * lax.rsqrt(mean_square + EPSILON) * gain


def whole_part(values, divisor):
    return jnp.floor((values + 0.5) / divisor)


def greet(n_seq, pairs):
    grp, seq = lax.axis_index("grp"), lax.axis_index("seq")
    barrier = pltpu.get_barrier_semaphore()
    for k in range(1, n_seq):
        pl.semaphore_signal(
            barrier, inc=1, device_id=(grp, lax.rem(seq + k, n_seq)), device_id_type=MESH
        )
    for other in pairs:
        pl.semaphore_signal(barrier, inc=1, device_id=(other, seq), device_id_type=MESH)
    pl.semaphore_wait(barrier, n_seq - 1 + len(pairs))


def flip(index, bit):
    return index + bit - 2 * bit * lax.rem(index // bit, 2)


class Relay:
    def __init__(self, n_seq, shard, full, first, local_sem, recv_sem, send_sem):
        self.n_seq, self.shard, self.full = n_seq, shard, full
        self.local_sem, self.recv_sem, self.send_sem = local_sem, recv_sem, send_sem
        self.line = n_seq // 2
        self.grp, self.seq = lax.axis_index("grp"), lax.axis_index("seq")
        self.place, self.side = self.seq // 2, lax.rem(self.seq, 2)
        far = flip(self.grp, 2)
        self.far = far
        across = flip(self.seq, 1)
        self.a_dev = (jnp.where(first, far, self.grp), jnp.where(first, self.seq, across))
        self.b_dev = (jnp.where(first, self.grp, far), jnp.where(first, across, self.seq))
        self.ab_dev = (far, across)
        self.core_dev = (flip(self.grp, 1), self.seq)

    def slot(self, base, place):
        return base[0] * self.n_seq + 2 * place + lax.rem(base[1], 2)

    def copy(self, slot, way, device, own=False):
        return pltpu.make_async_remote_copy(
            src_ref=self.shard if own else self.full.at[slot],
            dst_ref=self.full.at[slot],
            send_sem=self.send_sem.at[way, slot],
            recv_sem=self.recv_sem.at[slot],
            device_id=device,
            device_id_type=MESH,
        )

    def up(self):
        return (self.grp, jnp.minimum(self.seq + 2, self.n_seq - 2 + self.side))

    def down(self):
        return (self.grp, jnp.maximum(self.seq - 2, self.side))

    def me(self):
        return (self.grp, self.seq)

    def begin(self):
        slot = self.slot(self.me(), self.place)
        pltpu.make_async_copy(self.shard, self.full.at[slot], self.local_sem).start()

        @pl.when(self.place + 1 < self.line)
        def _():
            self.copy(slot, 0, self.up(), True).start()

        @pl.when(self.place > 0)
        def _():
            self.copy(slot, 1, self.down(), True).start()

        self.copy(slot, 2, self.a_dev, True).start()
        self.copy(slot, 3, self.b_dev, True).start()
        self.copy(slot, 4, self.core_dev, True).start()

    def spots(self, distance):
        low, high = self.place - distance, self.place + distance
        if distance == 0:
            return [(self.place, None, None)]
        return [(low, low >= 0, True), (high, high < self.line, False)]

    def visit(self, base, distance, ways, finish=False):
        for place, there, upward in self.spots(distance):

            def act(place=place, upward=upward):
                slot = self.slot(base, place)
                own_core = base is not None
                if not finish:
                    self.copy(slot, 4, self.core_dev).wait_recv()
                for way, device in ways:
                    move = self.copy(slot, way, device)
                    move.wait_send() if finish else move.start()
                if upward is True and "z" in self.mode:

                    @pl.when(self.place + 1 < self.line)
                    def _():
                        move = self.copy(slot, 0, self.up())
                        move.wait_send() if finish else move.start()

                if upward is False and "z" in self.mode:

                    @pl.when(self.place > 0)
                    def _():
                        move = self.copy(slot, 1, self.down())
                        move.wait_send() if finish else move.start()

            if there is None:
                act()
            else:
                pl.when(there)(act)

    def own_line(self, distance, finish=False):
        self.mode = "z"
        self.visit(
            self.me(), distance,
            [(2, self.a_dev), (3, self.b_dev), (4, self.core_dev)], finish,
        )

    def a_line(self, distance, finish=False):
        self.mode = ""
        self.visit(self.a_dev, distance, [(3, self.b_dev), (4, self.core_dev)], finish)

    def b_lines(self, distance, finish=False):
        self.mode = ""
        self.visit(self.b_dev, distance, [(4, self.core_dev)], finish)
        self.visit(self.ab_dev, distance, [(4, self.core_dev)], finish)

    def end(self):
        slot = self.slot(self.me(), self.place)

        @pl.when(self.place + 1 < self.line)
        def _():
            self.copy(slot, 0, self.up(), True).wait_send()

        @pl.when(self.place > 0)
        def _():
            self.copy(slot, 1, self.down(), True).wait_send()

        self.copy(slot, 2, self.a_dev, True).wait_send()
        self.copy(slot, 3, self.b_dev, True).wait_send()
        self.copy(slot, 4, self.core_dev, True).wait_send()
        for distance in range(self.line):
            if distance:
                self.own_line(distance, True)
            self.a_line(distance, True)
            self.b_lines(distance, True)

    def settle(self):
        slot = self.slot(self.me(), self.place)
        pltpu.make_async_copy(self.shard, self.full.at[slot], self.local_sem).wait()
        partner = self.core_dev[0]
        for place in range(self.line):
            for base in (
                (partner, self.seq), (partner, flip(self.seq, 1)),
                (flip(partner, 2), self.seq), (flip(partner, 2), flip(self.seq, 1)),
            ):
                slot = self.slot(base, place)
                self.copy(slot, 4, self.core_dev).wait_recv()


class Gather:
    def __init__(self, n_seq, buf, send_sem, recv_sem):
        self.buf, self.send_sem, self.recv_sem = buf, send_sem, recv_sem
        self.line = n_seq // 2
        self.grp, self.seq = lax.axis_index("grp"), lax.axis_index("seq")
        self.place, self.side = self.seq // 2, lax.rem(self.seq, 2)

    def copy(self, slot, way, place, device):
        return pltpu.make_async_remote_copy(
            src_ref=self.buf.at[slot],
            dst_ref=self.buf.at[slot],
            send_sem=self.send_sem.at[way, place],
            recv_sem=self.recv_sem.at[slot],
            device_id=device,
            device_id_type=MESH,
        )

    def across(self):
        return (self.grp, flip(self.seq, 1))

    def begin(self, finish=False):
        for place in range(self.line):

            @pl.when(self.place != place)
            def _():
                move = self.copy(self.seq, 0, place, (self.grp, 2 * place + self.side))
                move.wait_send() if finish else move.start()

        move = self.copy(self.seq, 1, self.place, self.across())
        move.wait_send() if finish else move.start()

    def forward(self, distance):
        low, high = self.place - distance, self.place + distance
        for place, there in ((low, low >= 0), (high, high < self.line)):

            @pl.when(there)
            def _():
                slot = 2 * place + self.side
                move = self.copy(slot, 1, place, self.across())
                move.wait_recv()
                move.start()

    def settle(self):
        for place in range(self.line):
            slot = 2 * place + 1 - self.side
            self.copy(slot, 1, place, self.across()).wait_recv()

    def end(self):
        self.begin(True)
        for place in range(self.line):

            @pl.when(self.place != place)
            def _():
                slot = 2 * place + self.side
                self.copy(slot, 1, place, self.across()).wait_send()


def relay_scratch(n_dev):
    return [
        pltpu.SemaphoreType.DMA,
        pltpu.SemaphoreType.DMA((n_dev,)),
        pltpu.SemaphoreType.DMA((5, n_dev)),
    ]


def swap(n_seq, send_of, land_of, send_sem, recv_sem):
    grp, seq = lax.axis_index("grp"), lax.axis_index("seq")
    moves = []
    for k in range(1, n_seq):
        to = lax.rem(seq + k, n_seq)
        moves.append(
            pltpu.make_async_remote_copy(
                src_ref=send_of(to),
                dst_ref=land_of(seq),
                send_sem=send_sem.at[k],
                recv_sem=recv_sem.at[k],
                device_id=(grp, to),
                device_id_type=MESH,
            )
        )
    for move in moves:
        move.start()
    return moves


def row_codes(dest, rows, capacity):
    order = lax.broadcasted_iota(jnp.int32, (rows, LANES), 0)
    target = jnp.zeros((rows, LANES), jnp.int32)
    for r in range(rows):
        target = jnp.where(order == r, dest[r], target)
    earlier = jnp.zeros((rows, LANES), jnp.int32)
    for r in range(rows):
        earlier = earlier + jnp.where((target == dest[r]) & (order > r), 1, 0)
    return (target * capacity + earlier).astype(jnp.float32)


def window_attention(projected, pieces, features):
    queries, keys, values = projected
    rows = queries.shape[0]
    head_dim = features // VHEADS
    together = LANES // math.gcd(LANES, head_dim)
    width = together * head_dim
    wide = jnp.broadcast_to(pieces.astype(jnp.float32), (rows, rows))
    allowed = wide == jnp.transpose(wide)
    lane = lax.broadcasted_iota(jnp.int32, (rows, width), 1)
    inside = [(lane >= h * head_dim) & (lane < (h + 1) * head_dim) for h in range(together)]
    parts = []
    for start in range(0, features, width):
        q = queries[:, start : start + width]
        stacked = jnp.concatenate(
            [jnp.where(inside[h], q, 0.0).astype(jnp.bfloat16) for h in range(together)], axis=0
        )
        scores = lax.dot_general(
            stacked, keys[:, start : start + width], (((1,), (1,)), ((), ())),
            preferred_element_type=jnp.float32,
        ) * head_dim ** (-0.5)
        scores = jnp.where(allowed[None], scores.reshape(together, rows, rows), -1e30)
        weights = jnp.exp(scores - jnp.max(scores, axis=-1, keepdims=True))
        totals = jnp.sum(weights, axis=-1, keepdims=True)
        mixed = jnp.dot(
            weights.reshape(together * rows, rows).astype(jnp.bfloat16),
            values[:, start : start + width],
            preferred_element_type=jnp.float32,
        )
        top = jnp.zeros((rows, width), jnp.float32)
        low = jnp.ones((rows, width), jnp.float32)
        for h in range(together):
            top = jnp.where(inside[h], mixed[h * rows : (h + 1) * rows], top)
            low = jnp.where(inside[h], totals[h], low)
        parts.append((top / low).astype(jnp.bfloat16))
    return jnp.concatenate(parts, axis=1)


def layer_kernel(
    n_grp, n_seq, capacity, reach,
    patches, pieces, vit_gain, merge_gain, attn_gain, image_index, dest, doc_lengths,
    vit_qkv, vit_out, merge_up, merge_down, tokens, attn_qkv, attn_out,
    result, out_all,
    wide_v, vit_out_v, up_v, down_v, qkv_all, normed_s, gathered, hidden, stage, landed,
    queries, kv, attended, out_v,
    load_sem, token_sem, result_sem, out_sem, gather_send, hidden_send, gather_recv, hidden_recv,
    table_send, table_recv, kv_send, kv_recv, *relay_sems,
):
    grp, seq = lax.axis_index("grp"), lax.axis_index("seq")
    bf16, f32 = jnp.bfloat16, jnp.float32
    rows, features = patches.shape
    tok_rows = tokens.shape[0]
    slots = n_seq * capacity
    part = features
    vit_loads = [
        pltpu.make_async_copy(
            vit_qkv.at[:, pl.ds(i * part, part)], wide_v.at[:, pl.ds(i * part, part)],
            load_sem.at[i],
        )
        for i in range(3)
    ]
    vit_out_load = pltpu.make_async_copy(vit_out, vit_out_v, load_sem.at[3])
    up_load = pltpu.make_async_copy(merge_up, up_v, load_sem.at[4])
    down_load = pltpu.make_async_copy(merge_down, down_v, load_sem.at[5])
    for load in vit_loads + [vit_out_load]:
        load.start()
    greet(n_seq, (flip(grp, 1), flip(grp, 2)))
    relay = Relay(n_seq, attn_qkv, qkv_all, False, *relay_sems[:3])
    relay.begin()

    chunk_width = merge_down.shape[1]
    per_row = vit_qkv.shape[1] // chunk_width

    def chunk(c):
        return wide_v.at[
            pl.ds((c // per_row) * tok_rows, tok_rows),
            pl.ds((c % per_row) * chunk_width, chunk_width),
        ]

    def chunk_columns(c):
        return pl.ds(c * chunk_width, chunk_width)

    residual = patches[...].astype(f32)
    normed = rms_scale(residual, vit_gain[...].reshape(1, features)).astype(bf16)
    projected = []
    for i in range(3):
        vit_loads[i].wait()
        projected.append(
            jnp.dot(
                normed, wide_v[:, i * part : (i + 1) * part], preferred_element_type=f32
            ).astype(bf16)
        )
    up_load.start()
    down_load.start()
    token_loads = [
        pltpu.make_async_copy(tokens.at[:, chunk_columns(c)], chunk(c), token_sem.at[c])
        for c in range(n_seq)
    ]
    mixture = window_attention(projected, pieces[...], features)
    vit_out_load.wait()
    residual = residual + jnp.dot(mixture, vit_out_v[...], preferred_element_type=f32)
    merged_in = rms_scale(residual, merge_gain[...].reshape(1, features))
    own = rows // 4
    pieces_of = features // LANES
    for j in range(pieces_of):
        normed_s[j] = merged_in[:, j * LANES : (j + 1) * LANES]
    for quarter in range(4):
        for j in range(pieces_of):
            start = quarter * features + j * LANES
            gathered[seq, :, start : start + LANES] = normed_s[
                j, pl.ds(quarter, own, stride=4), :
            ].astype(bf16)
    gathered[seq, :, 4 * features :] = row_codes(dest, own, capacity).astype(bf16)
    first = Gather(n_seq, gathered, gather_send, gather_recv)
    first.begin()
    relay.own_line(1)
    for load in token_loads:
        load.start()
    line = n_seq // 2
    for distance in range(1, line):
        first.forward(distance)
    for distance in range(2, line):
        relay.own_line(distance)
    relay.a_line(0)
    up_load.wait()
    first.settle()

    all_rows = n_seq * own
    entry = gathered[:, :, : 4 * features].reshape(all_rows, 4 * features)
    pre = jnp.dot(entry, up_v[...], preferred_element_type=f32)
    hidden[seq] = (0.5 * pre * (1.0 + lax.erf(pre * 0.5**0.5))).astype(bf16)
    second = Gather(n_seq, hidden, hidden_send, hidden_recv)
    second.begin()

    codes = gathered[:, :, 4 * features :].reshape(all_rows, LANES).astype(f32)[:, :1]
    row = lax.broadcasted_iota(jnp.int32, (all_rows, 1), 0).astype(f32)
    keys = codes + whole_part(row, own) * (n_seq * capacity)
    column = lax.broadcasted_iota(jnp.int32, (1, n_seq * slots), 1).astype(f32)
    target = whole_part(column, slots)
    place = column - target * slots
    source = whole_part(place, capacity)
    want = source * (n_seq * capacity) + target * capacity + place - source * capacity
    select = jnp.transpose(jnp.where(keys == want, 1.0, 0.0)).astype(bf16)

    for distance in range(1, line):
        second.forward(distance)
        relay.a_line(distance)
    down_load.wait()
    part_width = hidden.shape[2]

    def term(index):
        start = pl.multiple_of(index * part_width, 32)
        return jnp.dot(
            hidden[index], down_v[pl.ds(start, part_width), :], preferred_element_type=f32
        )

    side = lax.rem(seq, 2)
    total = term(side)
    for p in range(1, line):
        total = total + term(2 * p + side)
    second.settle()
    for p in range(line):
        total = total + term(2 * p + 1 - side)
    outgoing = jnp.dot(select, total.astype(bf16), preferred_element_type=f32).astype(bf16)
    stage[...] = outgoing.reshape(stage.shape)
    landed[seq] = stage[seq]
    table_moves = swap(
        n_seq, lambda to: stage.at[to], lambda me: landed.at[me], table_send, table_recv
    )
    out_relay = Relay(n_seq, attn_out, out_all, lax.rem(grp, 2) == 0, *relay_sems[3:])
    out_relay.begin()
    for distance in range(line):
        relay.b_lines(distance)

    slot = lax.broadcasted_iota(jnp.int32, (slots, tok_rows), 0)
    picked = jnp.where(slot == image_index[...].reshape(1, tok_rows), 1.0, 0.0)
    picker = jnp.transpose(picked)
    pictured = jnp.sum(picker, axis=1, keepdims=True) > 0.5
    picker = picker.astype(bf16)
    for move in table_moves:
        move.wait_recv()
    square = jnp.zeros((tok_rows, 1), f32)
    for c in range(n_seq):
        token_loads[c].wait()
        image = jnp.dot(picker, landed[c], preferred_element_type=f32)
        layer_in = jnp.where(pictured, image, chunk(c)[...].astype(f32))
        chunk(c)[...] = layer_in.astype(bf16)
        square = square + jnp.sum(layer_in * layer_in, axis=1, keepdims=True)
    out_relay.own_line(1)
    scale = lax.rsqrt(square / (n_seq * chunk_width) + EPSILON)
    relay.settle()
    shard_rows, qkv_width = attn_qkv.shape
    attn_projected = jnp.zeros((tok_rows, qkv_width), f32)
    for c in range(n_seq):
        gain = attn_gain[pl.ds(c * chunk_width, chunk_width)].reshape(1, chunk_width)
        tokens_in = (chunk(c)[...].astype(f32) * scale * gain).astype(bf16)
        weight = qkv_all[c * n_grp : (c + 1) * n_grp].reshape(n_grp * shard_rows, qkv_width)
        attn_projected = attn_projected + jnp.dot(tokens_in, weight, preferred_element_type=f32)
    query_width = attn_out.shape[0]
    queries[...] = attn_projected[:, :query_width].astype(bf16)
    kv[reach] = attn_projected[:, query_width:].astype(bf16)
    kv_moves = []
    for k in range(1, reach + 1):
        kv_moves.append(
            pltpu.make_async_remote_copy(
                src_ref=kv.at[reach],
                dst_ref=kv.at[reach - k],
                send_sem=kv_send.at[k],
                recv_sem=kv_recv.at[k],
                device_id=(grp, lax.rem(seq + k, n_seq)),
                device_id_type=MESH,
            )
        )
        pl.when(seq + k < n_seq)(kv_moves[-1].start)

        @pl.when(seq < k)
        def _():
            kv[reach - k] = jnp.zeros(kv.shape[1:], bf16)

    for distance in range(2, line):
        out_relay.own_line(distance)
    for distance in range(line):
        out_relay.a_line(distance)

    head_dim = kv.shape[2] // 2
    span = (reach + 1) * tok_rows
    position = seq * tok_rows + lax.broadcasted_iota(jnp.int32, (tok_rows, 1), 0)
    begins = jnp.zeros((tok_rows, 1), jnp.int32)
    total_length = jnp.int32(0)
    for k in range(doc_lengths.shape[1]):
        begins = jnp.where(position >= total_length, total_length, begins)
        total_length = total_length + doc_lengths[0, k]
    key_pos = (seq - reach) * tok_rows + lax.broadcasted_iota(jnp.int32, (tok_rows, span), 1)
    allowed = (key_pos >= begins) & (key_pos <= position)
    for k in range(1, reach + 1):
        pl.when(seq >= k)(kv_moves[k - 1].wait_recv)
    everything = kv[...].reshape(span, 2 * head_dim)
    keys, values = everything[:, :head_dim], everything[:, head_dim:]
    for h in range(query_width // head_dim):
        scores = lax.dot_general(
            queries[:, h * head_dim : (h + 1) * head_dim], keys,
            (((1,), (1,)), ((), ())), preferred_element_type=f32,
        ) * head_dim ** (-0.5)
        scores = jnp.where(allowed, scores, -1e30)
        weights = jnp.exp(scores - jnp.max(scores, axis=-1, keepdims=True))
        totals = jnp.sum(weights, axis=-1, keepdims=True)
        mixed = jnp.dot(weights.astype(bf16), values, preferred_element_type=f32)
        attended[:, h * head_dim : (h + 1) * head_dim] = (mixed / totals).astype(bf16)
    for distance in range(line):
        out_relay.b_lines(distance)
    out_relay.settle()

    n_dev = n_grp * n_seq
    out_width = attn_out.shape[1]
    out_loads = [
        pltpu.make_async_copy(out_all.at[i], out_v.at[i % AHEAD], out_sem.at[i % AHEAD])
        for i in range(n_dev)
    ]
    for i in range(AHEAD):
        out_loads[i].start()
    stores = []
    for c in range(n_seq):
        for j in range(n_grp):
            i = c * n_grp + j
            out_loads[i].wait()
            update = jnp.dot(attended[...], out_v[i % AHEAD], preferred_element_type=f32)
            if i + AHEAD < n_dev:
                out_loads[i + AHEAD].start()
            columns = slice(j * out_width, (j + 1) * out_width)
            held = chunk(c)
            held[:, columns] = (held[:, columns].astype(f32) + update).astype(bf16)
        stores.append(
            pltpu.make_async_copy(chunk(c), result.at[:, chunk_columns(c)], result_sem.at[c])
        )
        stores[-1].start()
    for store in stores:
        store.wait()
    first.end()
    second.end()
    for move in table_moves:
        move.wait_send()
    for k in range(1, reach + 1):
        pl.when(seq + k < n_seq)(kv_moves[k - 1].wait_send)
    relay.end()
    out_relay.end()


VMEM = pl.BlockSpec(memory_space=pltpu.VMEM)
SMEM = pl.BlockSpec(memory_space=pltpu.SMEM)
ANY = pl.BlockSpec(memory_space=pl.ANY)


def on_device(
    patches, piece_ids, vit_gain, vit_qkv, vit_out, merge_gain, merge_up, merge_down, dest,
    tokens, image_index, doc_lengths, attn_gain, attn_qkv, attn_out,
):
    rows, features = patches.shape
    n_seq, n_grp = lax.axis_size("seq"), lax.axis_size("grp")
    n_dev = n_seq * n_grp
    own = rows // 4
    capacity = own // (n_seq // 2)
    slots = n_seq * capacity
    reach = n_seq // 2
    line = n_seq // 2
    bf16, f32 = jnp.bfloat16, jnp.float32
    tok_rows = tokens.shape[0]
    query_width, out_width = attn_out.shape
    kv_width = attn_qkv.shape[1] - query_width
    down_width = merge_down.shape[1]
    dma = pltpu.SemaphoreType.DMA
    result, _ = pl.pallas_call(
        functools.partial(layer_kernel, n_grp, n_seq, capacity, reach),
        out_shape=(
            jax.ShapeDtypeStruct(tokens.shape, bf16),
            jax.ShapeDtypeStruct((n_dev,) + attn_out.shape, bf16),
        ),
        in_specs=[VMEM] * 6 + [SMEM] * 2 + [ANY] * 7,
        out_specs=(ANY, ANY),
        scratch_shapes=[
            pltpu.VMEM(vit_qkv.shape, bf16),
            pltpu.VMEM(vit_out.shape, bf16),
            pltpu.VMEM(merge_up.shape, bf16),
            pltpu.VMEM(merge_down.shape, bf16),
            pltpu.VMEM((n_dev,) + attn_qkv.shape, bf16),
            pltpu.VMEM((features // LANES, rows, LANES), f32),
            pltpu.VMEM((n_seq, own, 4 * features + LANES), bf16),
            pltpu.VMEM((n_seq, n_seq * own, merge_up.shape[1]), bf16),
            pltpu.VMEM((n_seq, slots, down_width), bf16),
            pltpu.VMEM((n_seq, slots, down_width), bf16),
            pltpu.VMEM((tok_rows, query_width), bf16),
            pltpu.VMEM((reach + 1, tok_rows, kv_width), bf16),
            pltpu.VMEM((tok_rows, query_width), bf16),
            pltpu.VMEM((AHEAD, query_width, out_width), bf16),
            dma((6,)), dma((n_seq,)), dma((n_seq,)), dma((AHEAD,)),
            dma((2, line)), dma((2, line)), dma((n_seq,)), dma((n_seq,)),
            dma((n_seq,)), dma((n_seq,)), dma((reach + 1,)), dma((reach + 1,)),
        ] + relay_scratch(n_dev) + relay_scratch(n_dev),
        compiler_params=pltpu.CompilerParams(
            collective_id=0, has_side_effects=True, vmem_limit_bytes=67000000
        ),
    )(
        patches, piece_ids, vit_gain, merge_gain, attn_gain, image_index, dest, doc_lengths,
        vit_qkv, vit_out, merge_up, merge_down, tokens, attn_qkv, attn_out,
    )
    return result


def solution(mesh):
    placed = (
        P(("grp", "seq"), None),
        P(("grp", "seq"), None),
        P(),
        P(),
        P(),
        P(),
        P(None, "seq"),
        P(None, "seq"),
        P(("grp", "seq")),
        P(("grp", "seq"), None),
        P(("grp", "seq")),
        P("grp", None),
        P(),
        P(("grp", "seq"), None),
        P(None, ("grp", "seq")),
    )
    return jax.shard_map(
        on_device, mesh=mesh, in_specs=placed, out_specs=P(("grp", "seq"), None), check_vma=False
    )
```

```python
import functools
import math

import jax
import jax.numpy as jnp
from jax import lax
from jax.experimental import pallas as pl
from jax.experimental.pallas import tpu as pltpu
from jax.sharding import PartitionSpec as P

VHEADS = 16
WIN = 64
LANES = 128
EPSILON = 1e-06
AHEAD = 8
PLAN = {0: ('wsx', 'ra0', 'ro1'), (1, 2): ('ro2',), 6: ('ra1', 'ro3', 'wsy', 'wsz', 'wsc'), (2, 2): ('ra2',), 10: ('ra3', 'wo1', 'wa0'), 11: ('rb0', 'rb1', 'rb2', 'rb3', 'wo2'), 12: ('wa1', 'wo3'), 13: ('wa2',), 14: ('wa3', 'wb0'), 16: ('wb1',), 17: ('wb2', 'wb3')}
MESH = pl.DeviceIdType.MESH


def rms_scale(inputs, gain):
    mean_square = jnp.mean(inputs * inputs, axis=-1, keepdims=True)
    return inputs * lax.rsqrt(mean_square + EPSILON) * gain


def whole_part(values, divisor):
    return jnp.floor((values + 0.5) / divisor)


def greet(n_seq, pairs):
    grp, seq = lax.axis_index("grp"), lax.axis_index("seq")
    barrier = pltpu.get_barrier_semaphore()
    for k in range(1, n_seq):
        pl.semaphore_signal(
            barrier, inc=1, device_id=(grp, lax.rem(seq + k, n_seq)), device_id_type=MESH
        )
    for other in pairs:
        pl.semaphore_signal(barrier, inc=1, device_id=(other, seq), device_id_type=MESH)
    pl.semaphore_wait(barrier, n_seq - 1 + len(pairs))


def flip(index, bit):
    return index + bit - 2 * bit * lax.rem(index // bit, 2)


class Relay:
    def __init__(self, n_seq, shard, full, first, plane, local_sem, recv_sem, send_sem):
        self.n_seq, self.shard, self.full = n_seq, shard, full
        self.local_sem, self.recv_sem, self.send_sem = local_sem, recv_sem, send_sem
        self.line = n_seq // 2
        self.grp, self.seq = lax.axis_index("grp"), lax.axis_index("seq")
        self.plane, self.first, self.done = plane, first, []
        self.place, self.side = self.seq // 2, lax.rem(self.seq, 2)
        far = flip(self.grp, 2)
        self.far = far
        across = flip(self.seq, 1)
        self.a_dev = (jnp.where(first, far, self.grp), jnp.where(first, self.seq, across))
        self.b_dev = (jnp.where(first, self.grp, far), jnp.where(first, across, self.seq))
        self.ab_dev = (far, across)
        self.core_dev = (flip(self.grp, 1), self.seq)

    def slot(self, base, place):
        return base[0] * self.n_seq + 2 * place + lax.rem(base[1], 2)

    def copy(self, slot, way, device, own=False):
        return pltpu.make_async_remote_copy(
            src_ref=self.shard if own else self.full.at[slot],
            dst_ref=self.full.at[slot],
            send_sem=self.send_sem.at[way, slot],
            recv_sem=self.recv_sem.at[slot],
            device_id=device,
            device_id_type=MESH,
        )

    def up(self):
        return (self.grp, jnp.minimum(self.seq + 2, self.n_seq - 2 + self.side))

    def down(self):
        return (self.grp, jnp.maximum(self.seq - 2, self.side))

    def me(self):
        return (self.grp, self.seq)

    def launch(self, kind):
        slot = self.slot(self.me(), self.place)
        if kind == "c":
            pltpu.make_async_copy(self.shard, self.full.at[slot], self.local_sem).start()
            self.copy(slot, 4, self.core_dev, True).start()
        elif kind == "z":

            @pl.when(self.place + 1 < self.line)
            def _():
                self.copy(slot, 0, self.up(), True).start()

            @pl.when(self.place > 0)
            def _():
                self.copy(slot, 1, self.down(), True).start()

        else:
            a_way = self.first if kind == "x" else jnp.logical_not(self.first)
            device = (self.far, self.seq) if kind == "x" else (self.grp, flip(self.seq, 1))
            self.copy(slot, jnp.where(a_way, 2, 3), device, True).start()

    def spots(self, distance):
        low, high = self.place - distance, self.place + distance
        if distance == 0:
            return [(self.place, None, None)]
        return [(low, low >= 0, True), (high, high < self.line, False)]

    def pass_on(self, slot, way, device, guard, finish):
        def act():
            move = self.copy(slot, way, device)
            move.wait_send() if finish else move.start()

        if guard is True:
            act()
        elif guard is not False:
            pl.when(guard)(act)

    def along(self, guard, room):
        if guard is True:
            return room
        return False if guard is False else guard & room

    def visit(self, base, distance, ways, line, finish=False):
        for place, there, upward in self.spots(distance):

            def act(place=place, upward=upward):
                slot = self.slot(base, place)
                if not finish:
                    self.copy(slot, 4, self.core_dev).wait_recv()
                if upward is not False:
                    room = self.along(line, self.place + 1 < self.line)
                    self.pass_on(slot, 0, self.up(), room, finish)
                if upward is not True:
                    room = self.along(line, self.place > 0)
                    self.pass_on(slot, 1, self.down(), room, finish)
                for way, device, guard in ways:
                    self.pass_on(slot, way, device, guard, finish)

            if there is None:
                act()
            else:
                pl.when(there)(act)

    def own_line(self, distance, finish=False):
        spread = self.plane
        beyond = (not spread) if isinstance(spread, bool) else jnp.logical_not(spread)
        ways = [(3, self.b_dev, True), (2, self.a_dev, beyond), (4, self.core_dev, True)]
        self.visit(self.me(), distance, ways, True, finish)

    def a_line(self, distance, finish=False):
        ways = [(3, self.b_dev, True), (4, self.core_dev, True)]
        self.visit(self.a_dev, distance, ways, self.plane, finish)

    def b_lines(self, distance, finish=False):
        ways = [(4, self.core_dev, True)]
        self.visit(self.b_dev, distance, ways, False, finish)
        self.visit(self.ab_dev, distance, ways, False, finish)

    def run(self, name):
        if name in self.done:
            return
        self.done.append(name)
        if name[0] == "s":
            self.launch(name[1])
        elif int(name[1:]) < self.line:
            actions = {"o": self.own_line, "a": self.a_line, "b": self.b_lines}
            actions[name[0]](int(name[1:]))

    def flush(self):
        for kind in "xyzc":
            self.run("s" + kind)
        for kind in "oab":
            for distance in range(kind == "o", self.line):
                self.run(kind + str(distance))

    def end(self):
        slot = self.slot(self.me(), self.place)

        @pl.when(self.place + 1 < self.line)
        def _():
            self.copy(slot, 0, self.up(), True).wait_send()

        @pl.when(self.place > 0)
        def _():
            self.copy(slot, 1, self.down(), True).wait_send()

        self.copy(slot, 2, self.a_dev, True).wait_send()
        self.copy(slot, 3, self.b_dev, True).wait_send()
        self.copy(slot, 4, self.core_dev, True).wait_send()
        for distance in range(self.line):
            if distance:
                self.own_line(distance, True)
            self.a_line(distance, True)
            self.b_lines(distance, True)

    def settle(self):
        slot = self.slot(self.me(), self.place)
        pltpu.make_async_copy(self.shard, self.full.at[slot], self.local_sem).wait()
        partner = self.core_dev[0]
        for place in range(self.line):
            for base in (
                (partner, self.seq), (partner, flip(self.seq, 1)),
                (flip(partner, 2), self.seq), (flip(partner, 2), flip(self.seq, 1)),
            ):
                slot = self.slot(base, place)
                self.copy(slot, 4, self.core_dev).wait_recv()


class Gather:
    def __init__(self, n_seq, buf, send_sem, recv_sem):
        self.buf, self.send_sem, self.recv_sem = buf, send_sem, recv_sem
        self.line = n_seq // 2
        self.grp, self.seq = lax.axis_index("grp"), lax.axis_index("seq")
        self.place, self.side = self.seq // 2, lax.rem(self.seq, 2)

    def copy(self, slot, way, place, device):
        return pltpu.make_async_remote_copy(
            src_ref=self.buf.at[slot],
            dst_ref=self.buf.at[slot],
            send_sem=self.send_sem.at[way, place],
            recv_sem=self.recv_sem.at[slot],
            device_id=device,
            device_id_type=MESH,
        )

    def across(self):
        return (self.grp, flip(self.seq, 1))

    def begin(self, finish=False):
        for place in range(self.line):

            @pl.when(self.place != place)
            def _():
                move = self.copy(self.seq, 0, place, (self.grp, 2 * place + self.side))
                move.wait_send() if finish else move.start()

        move = self.copy(self.seq, 1, self.place, self.across())
        move.wait_send() if finish else move.start()

    def forward(self, distance):
        low, high = self.place - distance, self.place + distance
        for place, there in ((low, low >= 0), (high, high < self.line)):

            @pl.when(there)
            def _():
                slot = 2 * place + self.side
                move = self.copy(slot, 1, place, self.across())
                move.wait_recv()
                move.start()

    def settle(self):
        for place in range(self.line):
            slot = 2 * place + 1 - self.side
            self.copy(slot, 1, place, self.across()).wait_recv()

    def end(self):
        self.begin(True)
        for place in range(self.line):

            @pl.when(self.place != place)
            def _():
                slot = 2 * place + self.side
                self.copy(slot, 1, place, self.across()).wait_send()


def relay_scratch(n_dev):
    return [
        pltpu.SemaphoreType.DMA,
        pltpu.SemaphoreType.DMA((n_dev,)),
        pltpu.SemaphoreType.DMA((5, n_dev)),
    ]


def swap(n_seq, send_of, land_of, send_sem, recv_sem):
    grp, seq = lax.axis_index("grp"), lax.axis_index("seq")
    moves = []
    for k in range(1, n_seq):
        to = lax.rem(seq + k, n_seq)
        moves.append(
            pltpu.make_async_remote_copy(
                src_ref=send_of(to),
                dst_ref=land_of(seq),
                send_sem=send_sem.at[k],
                recv_sem=recv_sem.at[k],
                device_id=(grp, to),
                device_id_type=MESH,
            )
        )
    for move in moves:
        move.start()
    return moves


def row_codes(dest, rows, capacity):
    order = lax.broadcasted_iota(jnp.int32, (rows, LANES), 0)
    target = jnp.zeros((rows, LANES), jnp.int32)
    for r in range(rows):
        target = jnp.where(order == r, dest[r], target)
    earlier = jnp.zeros((rows, LANES), jnp.int32)
    for r in range(rows):
        earlier = earlier + jnp.where((target == dest[r]) & (order > r), 1, 0)
    return (target * capacity + earlier).astype(jnp.float32)


def window_attention(projected, pieces, features):
    queries, keys, values = projected
    rows = queries.shape[0]
    head_dim = features // VHEADS
    together = LANES // math.gcd(LANES, head_dim)
    width = together * head_dim
    wide = jnp.broadcast_to(pieces.astype(jnp.float32), (rows, rows))
    allowed = wide == jnp.transpose(wide)
    lane = lax.broadcasted_iota(jnp.int32, (rows, width), 1)
    inside = [(lane >= h * head_dim) & (lane < (h + 1) * head_dim) for h in range(together)]
    parts = []
    for start in range(0, features, width):
        q = queries[:, start : start + width]
        stacked = jnp.concatenate(
            [jnp.where(inside[h], q, 0.0).astype(jnp.bfloat16) for h in range(together)], axis=0
        )
        scores = lax.dot_general(
            stacked, keys[:, start : start + width], (((1,), (1,)), ((), ())),
            preferred_element_type=jnp.float32,
        ) * head_dim ** (-0.5)
        scores = jnp.where(allowed[None], scores.reshape(together, rows, rows), -1e30)
        weights = jnp.exp(scores - jnp.max(scores, axis=-1, keepdims=True))
        totals = jnp.sum(weights, axis=-1, keepdims=True)
        mixed = jnp.dot(
            weights.reshape(together * rows, rows).astype(jnp.bfloat16),
            values[:, start : start + width],
            preferred_element_type=jnp.float32,
        )
        top = jnp.zeros((rows, width), jnp.float32)
        low = jnp.ones((rows, width), jnp.float32)
        for h in range(together):
            top = jnp.where(inside[h], mixed[h * rows : (h + 1) * rows], top)
            low = jnp.where(inside[h], totals[h], low)
        parts.append((top / low).astype(jnp.bfloat16))
    return jnp.concatenate(parts, axis=1)


def layer_kernel(
    n_grp, n_seq, capacity, reach,
    patches, pieces, vit_gain, merge_gain, attn_gain, image_index, dest, doc_lengths,
    vit_qkv, vit_out, merge_up, merge_down, tokens, attn_qkv, attn_out,
    result, out_all,
    wide_v, vit_out_v, up_v, down_v, qkv_all, normed_s, gathered, hidden, stage, landed,
    queries, kv, attended, out_v,
    load_sem, token_sem, result_sem, out_sem, gather_send, hidden_send, gather_recv, hidden_recv,
    table_send, table_recv, kv_send, kv_recv, *relay_sems,
):
    grp, seq = lax.axis_index("grp"), lax.axis_index("seq")
    bf16, f32 = jnp.bfloat16, jnp.float32
    rows, features = patches.shape
    tok_rows = tokens.shape[0]
    slots = n_seq * capacity
    part = features
    vit_loads = [
        pltpu.make_async_copy(
            vit_qkv.at[:, pl.ds(i * part, part)], wide_v.at[:, pl.ds(i * part, part)],
            load_sem.at[i],
        )
        for i in range(3)
    ]
    vit_out_load = pltpu.make_async_copy(vit_out, vit_out_v, load_sem.at[3])
    up_load = pltpu.make_async_copy(merge_up, up_v, load_sem.at[4])
    down_load = pltpu.make_async_copy(merge_down, down_v, load_sem.at[5])
    for load in vit_loads + [vit_out_load]:
        load.start()
    greet(n_seq, (flip(grp, 1), flip(grp, 2)))
    core = lax.rem(grp, 2)
    relay = Relay(n_seq, attn_qkv, qkv_all, False, False, *relay_sems[:3])
    for kind in "xyzc":
        relay.run("s" + kind)
    out_relay = Relay(n_seq, attn_out, out_all, core == 0, core == 1, *relay_sems[3:])

    def at(point):
        for name in PLAN.get(point, ()):
            (out_relay if name[0] == "w" else relay).run(name[1:])


    chunk_width = merge_down.shape[1]
    per_row = vit_qkv.shape[1] // chunk_width

    def chunk(c):
        return wide_v.at[
            pl.ds((c // per_row) * tok_rows, tok_rows),
            pl.ds((c % per_row) * chunk_width, chunk_width),
        ]

    def chunk_columns(c):
        return pl.ds(c * chunk_width, chunk_width)

    residual = patches[...].astype(f32)
    normed = rms_scale(residual, vit_gain[...].reshape(1, features)).astype(bf16)
    projected = []
    for i in range(3):
        vit_loads[i].wait()
        projected.append(
            jnp.dot(
                normed, wide_v[:, i * part : (i + 1) * part], preferred_element_type=f32
            ).astype(bf16)
        )
    up_load.start()
    down_load.start()
    token_loads = [
        pltpu.make_async_copy(tokens.at[:, chunk_columns(c)], chunk(c), token_sem.at[c])
        for c in range(n_seq)
    ]
    mixture = window_attention(projected, pieces[...], features)
    at(0)
    vit_out_load.wait()
    residual = residual + jnp.dot(mixture, vit_out_v[...], preferred_element_type=f32)
    merged_in = rms_scale(residual, merge_gain[...].reshape(1, features))
    own = rows // 4
    pieces_of = features // LANES
    for j in range(pieces_of):
        normed_s[j] = merged_in[:, j * LANES : (j + 1) * LANES]
    for quarter in range(4):
        for j in range(pieces_of):
            start = quarter * features + j * LANES
            gathered[seq, :, start : start + LANES] = normed_s[
                j, pl.ds(quarter, own, stride=4), :
            ].astype(bf16)
    gathered[seq, :, 4 * features :] = row_codes(dest, own, capacity).astype(bf16)
    first = Gather(n_seq, gathered, gather_send, gather_recv)
    first.begin()
    at(1)
    for load in token_loads:
        load.start()
    line = n_seq // 2
    for distance in range(1, line):
        first.forward(distance)
        at((1, distance))
    first.settle()
    at(5)
    up_load.wait()

    all_rows = n_seq * own
    entry = gathered[:, :, : 4 * features].reshape(all_rows, 4 * features)
    pre = jnp.dot(entry, up_v[...], preferred_element_type=f32)
    hidden[seq] = (0.5 * pre * (1.0 + lax.erf(pre * 0.5**0.5))).astype(bf16)
    second = Gather(n_seq, hidden, hidden_send, hidden_recv)
    second.begin()
    at(6)

    codes = gathered[:, :, 4 * features :].reshape(all_rows, LANES).astype(f32)[:, :1]
    row = lax.broadcasted_iota(jnp.int32, (all_rows, 1), 0).astype(f32)
    keys = codes + whole_part(row, own) * (n_seq * capacity)
    column = lax.broadcasted_iota(jnp.int32, (1, n_seq * slots), 1).astype(f32)
    target = whole_part(column, slots)
    place = column - target * slots
    source = whole_part(place, capacity)
    want = source * (n_seq * capacity) + target * capacity + place - source * capacity
    select = jnp.transpose(jnp.where(keys == want, 1.0, 0.0)).astype(bf16)

    for distance in range(1, line):
        second.forward(distance)
        at((2, distance))
    down_load.wait()
    part_width = hidden.shape[2]

    def term(index):
        start = pl.multiple_of(index * part_width, 32)
        return jnp.dot(
            hidden[index], down_v[pl.ds(start, part_width), :], preferred_element_type=f32
        )

    side = lax.rem(seq, 2)
    total = term(side)
    for p in range(1, line):
        total = total + term(2 * p + side)
    at(10)
    second.settle()
    for p in range(line):
        total = total + term(2 * p + 1 - side)
    outgoing = jnp.dot(select, total.astype(bf16), preferred_element_type=f32).astype(bf16)
    stage[...] = outgoing.reshape(stage.shape)
    landed[seq] = stage[seq]
    table_moves = swap(
        n_seq, lambda to: stage.at[to], lambda me: landed.at[me], table_send, table_recv
    )
    at(11)
    slot = lax.broadcasted_iota(jnp.int32, (slots, tok_rows), 0)
    picked = jnp.where(slot == image_index[...].reshape(1, tok_rows), 1.0, 0.0)
    picker = jnp.transpose(picked)
    pictured = jnp.sum(picker, axis=1, keepdims=True) > 0.5
    picker = picker.astype(bf16)
    for move in table_moves:
        move.wait_recv()
    at(12)
    square = jnp.zeros((tok_rows, 1), f32)
    for c in range(n_seq):
        token_loads[c].wait()
        image = jnp.dot(picker, landed[c], preferred_element_type=f32)
        layer_in = jnp.where(pictured, image, chunk(c)[...].astype(f32))
        chunk(c)[...] = layer_in.astype(bf16)
        square = square + jnp.sum(layer_in * layer_in, axis=1, keepdims=True)
    scale = lax.rsqrt(square / (n_seq * chunk_width) + EPSILON)
    at(13)
    relay.flush()
    relay.settle()
    shard_rows, qkv_width = attn_qkv.shape
    attn_projected = jnp.zeros((tok_rows, qkv_width), f32)
    for c in range(n_seq):
        gain = attn_gain[pl.ds(c * chunk_width, chunk_width)].reshape(1, chunk_width)
        tokens_in = (chunk(c)[...].astype(f32) * scale * gain).astype(bf16)
        weight = qkv_all[c * n_grp : (c + 1) * n_grp].reshape(n_grp * shard_rows, qkv_width)
        attn_projected = attn_projected + jnp.dot(tokens_in, weight, preferred_element_type=f32)
    query_width = attn_out.shape[0]
    queries[...] = attn_projected[:, :query_width].astype(bf16)
    kv[reach] = attn_projected[:, query_width:].astype(bf16)
    half = reach // 2
    post = seq // 2

    def kv_copy(k_from, k_to, way, device):
        return pltpu.make_async_remote_copy(
            src_ref=kv.at[reach - k_from],
            dst_ref=kv.at[reach - k_to],
            send_sem=kv_send.at[way],
            recv_sem=kv_recv.at[k_to],
            device_id=device,
            device_id_type=MESH,
        )

    mate = (grp, flip(seq, 1))
    kv_moves = [(side == 0, kv_copy(0, 1, 0, mate))]
    for d in range(1, half + 1):
        ahead = (grp, jnp.minimum(seq + 2 * d, n_seq - 1))
        kv_moves.append((post + d < line, kv_copy(0, 2 * d, d, ahead)))
    for there, move in kv_moves:
        pl.when(there)(move.start)
    for k in range(1, reach + 1):

        @pl.when(seq < k)
        def _():
            kv[reach - k] = jnp.zeros(kv.shape[1:], bf16)

    def kv_arrival(k):
        pl.when(seq >= k)(kv_copy(0, k, 0, mate).wait_recv)

    at(14)
    for d in range(1, half + 1):
        kv_arrival(2 * d)
        there = (post >= d) & ((side == 1) | (d < half))
        move = kv_copy(2 * d, jnp.minimum(2 * d + 1 - 2 * side, reach), half + d, mate)
        kv_moves.append((there, move))
        pl.when(there)(move.start)

    at(15)
    head_dim = kv.shape[2] // 2
    span = (reach + 1) * tok_rows
    at(16)
    position = seq * tok_rows + lax.broadcasted_iota(jnp.int32, (tok_rows, 1), 0)
    begins = jnp.zeros((tok_rows, 1), jnp.int32)
    total_length = jnp.int32(0)
    for k in range(doc_lengths.shape[1]):
        begins = jnp.where(position >= total_length, total_length, begins)
        total_length = total_length + doc_lengths[0, k]
    key_pos = (seq - reach) * tok_rows + lax.broadcasted_iota(jnp.int32, (tok_rows, span), 1)
    allowed = (key_pos >= begins) & (key_pos <= position)
    for k in range(1, reach, 2):
        kv_arrival(k)
    everything = kv[...].reshape(span, 2 * head_dim)
    keys, values = everything[:, :head_dim], everything[:, head_dim:]
    for h in range(query_width // head_dim):
        scores = lax.dot_general(
            queries[:, h * head_dim : (h + 1) * head_dim], keys,
            (((1,), (1,)), ((), ())), preferred_element_type=f32,
        ) * head_dim ** (-0.5)
        scores = jnp.where(allowed, scores, -1e30)
        weights = jnp.exp(scores - jnp.max(scores, axis=-1, keepdims=True))
        totals = jnp.sum(weights, axis=-1, keepdims=True)
        mixed = jnp.dot(weights.astype(bf16), values, preferred_element_type=f32)
        attended[:, h * head_dim : (h + 1) * head_dim] = (mixed / totals).astype(bf16)
    at(17)
    out_relay.flush()
    out_relay.settle()

    n_dev = n_grp * n_seq
    out_width = attn_out.shape[1]
    streamed = out_width % LANES != 0
    ahead = AHEAD if streamed else 0
    out_loads = [
        pltpu.make_async_copy(out_all.at[i], out_v.at[i % AHEAD], out_sem.at[i % AHEAD])
        for i in range(n_dev if streamed else 0)
    ]
    for i in range(ahead):
        out_loads[i].start()
    stores = []
    for c in range(n_seq):
        for j in range(n_grp):
            i = c * n_grp + j
            if streamed:
                out_loads[i].wait()
            weight = out_v[i % AHEAD] if streamed else out_all[i]
            update = jnp.dot(attended[...], weight, preferred_element_type=f32)
            if streamed and i + AHEAD < n_dev:
                out_loads[i + AHEAD].start()
            columns = slice(j * out_width, (j + 1) * out_width)
            held = chunk(c)
            held[:, columns] = (held[:, columns].astype(f32) + update).astype(bf16)
        stores.append(
            pltpu.make_async_copy(chunk(c), result.at[:, chunk_columns(c)], result_sem.at[c])
        )
        stores[-1].start()
    for store in stores:
        store.wait()
    first.end()
    second.end()
    for move in table_moves:
        move.wait_send()
    for there, move in kv_moves:
        pl.when(there)(move.wait_send)
    relay.end()
    out_relay.end()


VMEM = pl.BlockSpec(memory_space=pltpu.VMEM)
SMEM = pl.BlockSpec(memory_space=pltpu.SMEM)
ANY = pl.BlockSpec(memory_space=pl.ANY)


def on_device(
    patches, piece_ids, vit_gain, vit_qkv, vit_out, merge_gain, merge_up, merge_down, dest,
    tokens, image_index, doc_lengths, attn_gain, attn_qkv, attn_out,
):
    rows, features = patches.shape
    n_seq, n_grp = lax.axis_size("seq"), lax.axis_size("grp")
    n_dev = n_seq * n_grp
    own = rows // 4
    capacity = own // (n_seq // 2)
    slots = n_seq * capacity
    reach = n_seq // 2
    line = n_seq // 2
    bf16, f32 = jnp.bfloat16, jnp.float32
    tok_rows = tokens.shape[0]
    query_width, out_width = attn_out.shape
    kv_width = attn_qkv.shape[1] - query_width
    down_width = merge_down.shape[1]
    dma = pltpu.SemaphoreType.DMA
    streamed = out_width % LANES != 0
    out_all_shape = (n_dev,) + attn_out.shape
    outputs = [jax.ShapeDtypeStruct(tokens.shape, bf16)]
    held = [pltpu.VMEM(out_all_shape, bf16)]
    if streamed:
        outputs.append(jax.ShapeDtypeStruct(out_all_shape, bf16))
        held = []
    results = pl.pallas_call(
        functools.partial(layer_kernel, n_grp, n_seq, capacity, reach),
        out_shape=tuple(outputs),
        in_specs=[VMEM] * 6 + [SMEM] * 2 + [ANY] * 7,
        out_specs=(ANY,) * len(outputs),
        scratch_shapes=held + [
            pltpu.VMEM(vit_qkv.shape, bf16),
            pltpu.VMEM(vit_out.shape, bf16),
            pltpu.VMEM(merge_up.shape, bf16),
            pltpu.VMEM(merge_down.shape, bf16),
            pltpu.VMEM((n_dev,) + attn_qkv.shape, bf16),
            pltpu.VMEM((features // LANES, rows, LANES), f32),
            pltpu.VMEM((n_seq, own, 4 * features + LANES), bf16),
            pltpu.VMEM((n_seq, n_seq * own, merge_up.shape[1]), bf16),
            pltpu.VMEM((n_seq, slots, down_width), bf16),
            pltpu.VMEM((n_seq, slots, down_width), bf16),
            pltpu.VMEM((tok_rows, query_width), bf16),
            pltpu.VMEM((reach + 1, tok_rows, kv_width), bf16),
            pltpu.VMEM((tok_rows, query_width), bf16),
            pltpu.VMEM((AHEAD, query_width if streamed else 16, out_width), bf16),
            dma((6,)), dma((n_seq,)), dma((n_seq,)), dma((AHEAD,)),
            dma((2, line)), dma((2, line)), dma((n_seq,)), dma((n_seq,)),
            dma((n_seq,)), dma((n_seq,)), dma((reach + 2,)), dma((reach + 1,)),
        ] + relay_scratch(n_dev) + relay_scratch(n_dev),
        compiler_params=pltpu.CompilerParams(
            collective_id=0, has_side_effects=True, vmem_limit_bytes=67043328
        ),
    )(
        patches, piece_ids, vit_gain, merge_gain, attn_gain, image_index, dest, doc_lengths,
        vit_qkv, vit_out, merge_up, merge_down, tokens, attn_qkv, attn_out,
    )
    return results[0]


def solution(mesh):
    placed = (
        P(("grp", "seq"), None),
        P(("grp", "seq"), None),
        P(),
        P(),
        P(),
        P(),
        P(None, "seq"),
        P(None, "seq"),
        P(("grp", "seq")),
        P(("grp", "seq"), None),
        P(("grp", "seq")),
        P("grp", None),
        P(),
        P(("grp", "seq"), None),
        P(None, ("grp", "seq")),
    )
    return jax.shard_map(
        on_device, mesh=mesh, in_specs=placed, out_specs=P(("grp", "seq"), None), check_vma=False
    )
```

```python
import functools
import math

import jax
import jax.numpy as jnp
from jax import lax
from jax.experimental import pallas as pl
from jax.experimental.pallas import tpu as pltpu
from jax.sharding import PartitionSpec as P

VHEADS = 16
WIN = 64
LANES = 128
EPSILON = 1e-06
AHEAD = 8
PLAN = {0: ('wsx', 'ra0', 'ro1xc'), 1: ('ro1z', 'ro1y'), (1, 2): ('ro2',), 6: ('ra1', 'ro3', 'wsy', 'wsz', 'wsc'), (2, 2): ('ra2',), 10: ('ra3', 'wo1', 'wa0'), 11: ('rb0', 'rb1', 'rb2', 'rb3', 'wo2'), 12: ('wa1', 'wo3'), 14: ('wa2',), 15: ('wa3',), 16: ('wb0', 'wb1'), 17: ('wb2', 'wb3')}
MESH = pl.DeviceIdType.MESH


def rms_scale(inputs, gain):
    mean_square = jnp.mean(inputs * inputs, axis=-1, keepdims=True)
    return inputs * lax.rsqrt(mean_square + EPSILON) * gain


def whole_part(values, divisor):
    return jnp.floor((values + 0.5) / divisor)


def greet(n_seq, pairs):
    grp, seq = lax.axis_index("grp"), lax.axis_index("seq")
    barrier = pltpu.get_barrier_semaphore()
    for k in range(1, n_seq):
        pl.semaphore_signal(
            barrier, inc=1, device_id=(grp, lax.rem(seq + k, n_seq)), device_id_type=MESH
        )
    for other in pairs:
        pl.semaphore_signal(barrier, inc=1, device_id=(other, seq), device_id_type=MESH)
    pl.semaphore_wait(barrier, n_seq - 1 + len(pairs))


def flip(index, bit):
    return index + bit - 2 * bit * lax.rem(index // bit, 2)


def opposite(flag):
    return (not flag) if isinstance(flag, bool) else jnp.logical_not(flag)


def either(left, right):
    if left is True or right is True:
        return True
    if left is False:
        return right
    return left if right is False else left | right


def both(left, right):
    if left is False or right is False:
        return False
    if left is True:
        return right
    return left if right is True else left & right


class Relay:
    def __init__(self, n_seq, shard, full, first, plane, local_sem, recv_sem, send_sem):
        self.n_seq, self.shard, self.full = n_seq, shard, full
        self.local_sem, self.recv_sem, self.send_sem = local_sem, recv_sem, send_sem
        self.line = n_seq // 2
        self.grp, self.seq = lax.axis_index("grp"), lax.axis_index("seq")
        self.plane, self.first, self.done = plane, first, []
        self.place, self.side = self.seq // 2, lax.rem(self.seq, 2)
        far = flip(self.grp, 2)
        self.far = far
        across = flip(self.seq, 1)
        self.a_dev = (jnp.where(first, far, self.grp), jnp.where(first, self.seq, across))
        self.b_dev = (jnp.where(first, self.grp, far), jnp.where(first, across, self.seq))
        self.ab_dev = (far, across)
        self.core_dev = (flip(self.grp, 1), self.seq)

    def slot(self, base, place):
        return base[0] * self.n_seq + 2 * place + lax.rem(base[1], 2)

    def copy(self, slot, way, device, own=False):
        return pltpu.make_async_remote_copy(
            src_ref=self.shard if own else self.full.at[slot],
            dst_ref=self.full.at[slot],
            send_sem=self.send_sem.at[way, slot],
            recv_sem=self.recv_sem.at[slot],
            device_id=device,
            device_id_type=MESH,
        )

    def up(self):
        return (self.grp, jnp.minimum(self.seq + 2, self.n_seq - 2 + self.side))

    def down(self):
        return (self.grp, jnp.maximum(self.seq - 2, self.side))

    def me(self):
        return (self.grp, self.seq)

    def launch(self, kind):
        slot = self.slot(self.me(), self.place)
        if kind == "c":
            pltpu.make_async_copy(self.shard, self.full.at[slot], self.local_sem).start()
            self.copy(slot, 4, self.core_dev, True).start()
        elif kind == "z":

            @pl.when(self.place + 1 < self.line)
            def _():
                self.copy(slot, 0, self.up(), True).start()

            @pl.when(self.place > 0)
            def _():
                self.copy(slot, 1, self.down(), True).start()

        else:
            way, device = self.side_way(kind)
            self.copy(slot, way, device, True).start()

    def spots(self, distance):
        low, high = self.place - distance, self.place + distance
        if distance == 0:
            return [(self.place, None, None)]
        return [(low, low >= 0, True), (high, high < self.line, False)]

    def pass_on(self, slot, way, device, guard, finish):
        def act():
            move = self.copy(slot, way, device)
            move.wait_send() if finish else move.start()

        if guard is True:
            act()
        elif guard is not False:
            pl.when(guard)(act)

    def visit(self, base, distance, ways, finish):
        for place, there, upward in self.spots(distance):

            def act(place=place, upward=upward):
                slot = self.slot(base, place)
                for kind, guard in ways:
                    if kind == "r":
                        self.copy(slot, 4, self.core_dev).wait_recv()
                    elif kind == "z":
                        if upward is not False:
                            room = both(guard, self.place + 1 < self.line)
                            self.pass_on(slot, 0, self.up(), room, finish)
                        if upward is not True:
                            room = both(guard, self.place > 0)
                            self.pass_on(slot, 1, self.down(), room, finish)
                    elif kind == "c":
                        self.pass_on(slot, 4, self.core_dev, guard, finish)
                    else:
                        self.pass_on(slot, *self.side_way(kind), guard, finish)

            if there is None:
                act()
            else:
                pl.when(there)(act)

    def side_way(self, kind):
        a_way = self.first if kind == "x" else opposite(self.first)
        device = (self.far, self.seq) if kind == "x" else (self.grp, flip(self.seq, 1))
        return jnp.where(a_way, 2, 3), device

    def forward(self, kind, distance, ways, finish=False):
        later = opposite(self.plane)
        guards = {
            "o": {
                "x": either(opposite(self.first), later), "y": either(self.first, later),
                "z": True, "c": True,
            },
            "a": {"x": opposite(self.first), "y": self.first, "z": self.plane, "c": True},
            "b": {"c": True},
        }[kind]
        chosen = [("r", True)] if "r" in ways else []
        chosen += [(way, guards[way]) for way in ways if way in guards]
        bases = {"o": [self.me()], "a": [self.a_dev], "b": [self.b_dev, self.ab_dev]}[kind]
        for base in bases:
            self.visit(base, distance, chosen, finish)

    def run(self, name):
        if name[0] == "s":
            if name not in self.done:
                self.launch(name[1])
            self.done.append(name)
            return
        kind, distance = name[0], int(name[1])
        self.run_ways(kind, distance, name[2:] or "xyzc")

    def run_ways(self, kind, distance, ways):
        if distance >= self.line:
            return
        ways = [way for way in "r" + ways if (kind, distance, way) not in self.done]
        self.done += [(kind, distance, way) for way in ways]
        if ways:
            self.forward(kind, distance, ways)

    def flush(self):
        for kind in "xyzc":
            self.run("s" + kind)
        for kind in "oab":
            for distance in range(kind == "o", self.line):
                self.run_ways(kind, distance, "xyzc")

    def end(self):
        slot = self.slot(self.me(), self.place)

        @pl.when(self.place + 1 < self.line)
        def _():
            self.copy(slot, 0, self.up(), True).wait_send()

        @pl.when(self.place > 0)
        def _():
            self.copy(slot, 1, self.down(), True).wait_send()

        self.copy(slot, 2, self.a_dev, True).wait_send()
        self.copy(slot, 3, self.b_dev, True).wait_send()
        self.copy(slot, 4, self.core_dev, True).wait_send()
        for kind in "oab":
            for distance in range(kind == "o", self.line):
                self.forward(kind, distance, "xyzc", True)

    def settle(self):
        slot = self.slot(self.me(), self.place)
        pltpu.make_async_copy(self.shard, self.full.at[slot], self.local_sem).wait()
        partner = self.core_dev[0]
        for place in range(self.line):
            for base in (
                (partner, self.seq), (partner, flip(self.seq, 1)),
                (flip(partner, 2), self.seq), (flip(partner, 2), flip(self.seq, 1)),
            ):
                slot = self.slot(base, place)
                self.copy(slot, 4, self.core_dev).wait_recv()


class Gather:
    def __init__(self, n_seq, buf, send_sem, recv_sem):
        self.buf, self.send_sem, self.recv_sem = buf, send_sem, recv_sem
        self.line = n_seq // 2
        self.grp, self.seq = lax.axis_index("grp"), lax.axis_index("seq")
        self.place, self.side = self.seq // 2, lax.rem(self.seq, 2)

    def copy(self, slot, way, place, device):
        return pltpu.make_async_remote_copy(
            src_ref=self.buf.at[slot],
            dst_ref=self.buf.at[slot],
            send_sem=self.send_sem.at[way, place],
            recv_sem=self.recv_sem.at[slot],
            device_id=device,
            device_id_type=MESH,
        )

    def across(self):
        return (self.grp, flip(self.seq, 1))

    def begin(self, finish=False):
        for place in range(self.line):

            @pl.when(self.place != place)
            def _():
                move = self.copy(self.seq, 0, place, (self.grp, 2 * place + self.side))
                move.wait_send() if finish else move.start()

        move = self.copy(self.seq, 1, self.place, self.across())
        move.wait_send() if finish else move.start()

    def forward(self, distance):
        low, high = self.place - distance, self.place + distance
        for place, there in ((low, low >= 0), (high, high < self.line)):

            @pl.when(there)
            def _():
                slot = 2 * place + self.side
                move = self.copy(slot, 1, place, self.across())
                move.wait_recv()
                move.start()

    def settle(self):
        for place in range(self.line):
            slot = 2 * place + 1 - self.side
            self.copy(slot, 1, place, self.across()).wait_recv()

    def end(self):
        self.begin(True)
        for place in range(self.line):

            @pl.when(self.place != place)
            def _():
                slot = 2 * place + self.side
                self.copy(slot, 1, place, self.across()).wait_send()


def relay_scratch(n_dev):
    return [
        pltpu.SemaphoreType.DMA,
        pltpu.SemaphoreType.DMA((n_dev,)),
        pltpu.SemaphoreType.DMA((5, n_dev)),
    ]


def swap(n_seq, send_of, land_of, send_sem, recv_sem):
    grp, seq = lax.axis_index("grp"), lax.axis_index("seq")
    moves = []
    for k in range(1, n_seq):
        to = lax.rem(seq + k, n_seq)
        moves.append(
            pltpu.make_async_remote_copy(
                src_ref=send_of(to),
                dst_ref=land_of(seq),
                send_sem=send_sem.at[k],
                recv_sem=recv_sem.at[k],
                device_id=(grp, to),
                device_id_type=MESH,
            )
        )
    for move in moves:
        move.start()
    return moves


def row_codes(dest, rows, capacity):
    order = lax.broadcasted_iota(jnp.int32, (rows, LANES), 0)
    target = jnp.zeros((rows, LANES), jnp.int32)
    for r in range(rows):
        target = jnp.where(order == r, dest[r], target)
    earlier = jnp.zeros((rows, LANES), jnp.int32)
    for r in range(rows):
        earlier = earlier + jnp.where((target == dest[r]) & (order > r), 1, 0)
    return (target * capacity + earlier).astype(jnp.float32)


def window_attention(projected, pieces, features):
    queries, keys, values = projected
    rows = queries.shape[0]
    head_dim = features // VHEADS
    together = LANES // math.gcd(LANES, head_dim)
    width = together * head_dim
    wide = jnp.broadcast_to(pieces.astype(jnp.float32), (rows, rows))
    allowed = wide == jnp.transpose(wide)
    lane = lax.broadcasted_iota(jnp.int32, (rows, width), 1)
    inside = [(lane >= h * head_dim) & (lane < (h + 1) * head_dim) for h in range(together)]
    parts = []
    for start in range(0, features, width):
        q = queries[:, start : start + width]
        stacked = jnp.concatenate(
            [jnp.where(inside[h], q, 0.0).astype(jnp.bfloat16) for h in range(together)], axis=0
        )
        scores = lax.dot_general(
            stacked, keys[:, start : start + width], (((1,), (1,)), ((), ())),
            preferred_element_type=jnp.float32,
        ) * head_dim ** (-0.5)
        scores = jnp.where(allowed[None], scores.reshape(together, rows, rows), -1e30)
        weights = jnp.exp(scores - jnp.max(scores, axis=-1, keepdims=True))
        totals = jnp.sum(weights, axis=-1, keepdims=True)
        mixed = jnp.dot(
            weights.reshape(together * rows, rows).astype(jnp.bfloat16),
            values[:, start : start + width],
            preferred_element_type=jnp.float32,
        )
        top = jnp.zeros((rows, width), jnp.float32)
        low = jnp.ones((rows, width), jnp.float32)
        for h in range(together):
            top = jnp.where(inside[h], mixed[h * rows : (h + 1) * rows], top)
            low = jnp.where(inside[h], totals[h], low)
        parts.append((top / low).astype(jnp.bfloat16))
    return jnp.concatenate(parts, axis=1)


def layer_kernel(
    n_grp, n_seq, capacity, reach,
    patches, pieces, vit_gain, merge_gain, attn_gain, image_index, dest, doc_lengths,
    vit_qkv, vit_out, merge_up, merge_down, tokens, attn_qkv, attn_out,
    result, out_all,
    wide_v, vit_out_v, up_v, down_v, qkv_all, normed_s, gathered, hidden, stage, landed,
    queries, kv, attended, out_v,
    load_sem, token_sem, result_sem, out_sem, gather_send, hidden_send, gather_recv, hidden_recv,
    table_send, table_recv, kv_send, kv_recv, *relay_sems,
):
    grp, seq = lax.axis_index("grp"), lax.axis_index("seq")
    bf16, f32 = jnp.bfloat16, jnp.float32
    rows, features = patches.shape
    tok_rows = tokens.shape[0]
    slots = n_seq * capacity
    part = features
    vit_loads = [
        pltpu.make_async_copy(
            vit_qkv.at[:, pl.ds(i * part, part)], wide_v.at[:, pl.ds(i * part, part)],
            load_sem.at[i],
        )
        for i in range(3)
    ]
    vit_out_load = pltpu.make_async_copy(vit_out, vit_out_v, load_sem.at[3])
    up_load = pltpu.make_async_copy(merge_up, up_v, load_sem.at[4])
    down_load = pltpu.make_async_copy(merge_down, down_v, load_sem.at[5])
    for load in vit_loads + [vit_out_load]:
        load.start()
    greet(n_seq, (flip(grp, 1), flip(grp, 2)))
    core = lax.rem(grp, 2)
    relay = Relay(n_seq, attn_qkv, qkv_all, False, False, *relay_sems[:3])
    for kind in "xyzc":
        relay.run("s" + kind)
    out_relay = Relay(n_seq, attn_out, out_all, core == 0, core == 1, *relay_sems[3:])

    def at(point):
        for name in PLAN.get(point, ()):
            (out_relay if name[0] == "w" else relay).run(name[1:])


    chunk_width = merge_down.shape[1]
    per_row = vit_qkv.shape[1] // chunk_width

    def chunk(c):
        return wide_v.at[
            pl.ds((c // per_row) * tok_rows, tok_rows),
            pl.ds((c % per_row) * chunk_width, chunk_width),
        ]

    def chunk_columns(c):
        return pl.ds(c * chunk_width, chunk_width)

    residual = patches[...].astype(f32)
    normed = rms_scale(residual, vit_gain[...].reshape(1, features)).astype(bf16)
    projected = []
    for i in range(3):
        vit_loads[i].wait()
        projected.append(
            jnp.dot(
                normed, wide_v[:, i * part : (i + 1) * part], preferred_element_type=f32
            ).astype(bf16)
        )
    up_load.start()
    down_load.start()
    token_loads = [
        pltpu.make_async_copy(tokens.at[:, chunk_columns(c)], chunk(c), token_sem.at[c])
        for c in range(n_seq)
    ]
    mixture = window_attention(projected, pieces[...], features)
    at(0)
    vit_out_load.wait()
    residual = residual + jnp.dot(mixture, vit_out_v[...], preferred_element_type=f32)
    merged_in = rms_scale(residual, merge_gain[...].reshape(1, features))
    own = rows // 4
    pieces_of = features // LANES
    for j in range(pieces_of):
        normed_s[j] = merged_in[:, j * LANES : (j + 1) * LANES]
    for quarter in range(4):
        for j in range(pieces_of):
            start = quarter * features + j * LANES
            gathered[seq, :, start : start + LANES] = normed_s[
                j, pl.ds(quarter, own, stride=4), :
            ].astype(bf16)
    gathered[seq, :, 4 * features :] = row_codes(dest, own, capacity).astype(bf16)
    first = Gather(n_seq, gathered, gather_send, gather_recv)
    first.begin()
    at(1)
    for load in token_loads:
        load.start()
    line = n_seq // 2
    for distance in range(1, line):
        first.forward(distance)
        at((1, distance))
    first.settle()
    at(5)
    up_load.wait()

    all_rows = n_seq * own
    entry = gathered[:, :, : 4 * features].reshape(all_rows, 4 * features)
    pre = jnp.dot(entry, up_v[...], preferred_element_type=f32)
    hidden[seq] = (0.5 * pre * (1.0 + lax.erf(pre * 0.5**0.5))).astype(bf16)
    second = Gather(n_seq, hidden, hidden_send, hidden_recv)
    second.begin()
    at(6)

    codes = gathered[:, :, 4 * features :].reshape(all_rows, LANES).astype(f32)[:, :1]
    row = lax.broadcasted_iota(jnp.int32, (all_rows, 1), 0).astype(f32)
    keys = codes + whole_part(row, own) * (n_seq * capacity)
    column = lax.broadcasted_iota(jnp.int32, (1, n_seq * slots), 1).astype(f32)
    target = whole_part(column, slots)
    place = column - target * slots
    source = whole_part(place, capacity)
    want = source * (n_seq * capacity) + target * capacity + place - source * capacity
    select = jnp.transpose(jnp.where(keys == want, 1.0, 0.0)).astype(bf16)

    for distance in range(1, line):
        second.forward(distance)
        at((2, distance))
    down_load.wait()
    part_width = hidden.shape[2]

    def term(index):
        start = pl.multiple_of(index * part_width, 32)
        return jnp.dot(
            hidden[index], down_v[pl.ds(start, part_width), :], preferred_element_type=f32
        )

    side = lax.rem(seq, 2)
    total = term(side)
    for p in range(1, line):
        total = total + term(2 * p + side)
    at(10)
    second.settle()
    for p in range(line):
        total = total + term(2 * p + 1 - side)
    outgoing = jnp.dot(select, total.astype(bf16), preferred_element_type=f32).astype(bf16)
    stage[...] = outgoing.reshape(stage.shape)
    landed[seq] = stage[seq]
    table_moves = swap(
        n_seq, lambda to: stage.at[to], lambda me: landed.at[me], table_send, table_recv
    )
    at(11)
    slot = lax.broadcasted_iota(jnp.int32, (slots, tok_rows), 0)
    picked = jnp.where(slot == image_index[...].reshape(1, tok_rows), 1.0, 0.0)
    picker = jnp.transpose(picked)
    pictured = jnp.sum(picker, axis=1, keepdims=True) > 0.5
    picker = picker.astype(bf16)
    for move in table_moves:
        move.wait_recv()
    at(12)
    square = jnp.zeros((tok_rows, 1), f32)
    for c in range(n_seq):
        token_loads[c].wait()
        image = jnp.dot(picker, landed[c], preferred_element_type=f32)
        layer_in = jnp.where(pictured, image, chunk(c)[...].astype(f32))
        chunk(c)[...] = layer_in.astype(bf16)
        square = square + jnp.sum(layer_in * layer_in, axis=1, keepdims=True)
    scale = lax.rsqrt(square / (n_seq * chunk_width) + EPSILON)
    at(13)
    relay.flush()
    relay.settle()
    shard_rows, qkv_width = attn_qkv.shape
    attn_projected = jnp.zeros((tok_rows, qkv_width), f32)
    for c in range(n_seq):
        gain = attn_gain[pl.ds(c * chunk_width, chunk_width)].reshape(1, chunk_width)
        tokens_in = (chunk(c)[...].astype(f32) * scale * gain).astype(bf16)
        weight = qkv_all[c * n_grp : (c + 1) * n_grp].reshape(n_grp * shard_rows, qkv_width)
        attn_projected = attn_projected + jnp.dot(tokens_in, weight, preferred_element_type=f32)
    query_width = attn_out.shape[0]
    queries[...] = attn_projected[:, :query_width].astype(bf16)
    kv[reach] = attn_projected[:, query_width:].astype(bf16)
    half = reach // 2
    post = seq // 2

    def kv_copy(k_from, k_to, way, device):
        return pltpu.make_async_remote_copy(
            src_ref=kv.at[reach - k_from],
            dst_ref=kv.at[reach - k_to],
            send_sem=kv_send.at[way],
            recv_sem=kv_recv.at[k_to],
            device_id=device,
            device_id_type=MESH,
        )

    mate = (grp, flip(seq, 1))
    kv_moves = [(side == 0, kv_copy(0, 1, 0, mate))]
    for d in range(1, half + 1):
        ahead = (grp, jnp.minimum(seq + 2 * d, n_seq - 1))
        kv_moves.append((post + d < line, kv_copy(0, 2 * d, d, ahead)))
    for there, move in kv_moves:
        pl.when(there)(move.start)
    for k in range(1, reach + 1):

        @pl.when(seq < k)
        def _():
            kv[reach - k] = jnp.zeros(kv.shape[1:], bf16)

    def kv_arrival(k):
        pl.when(seq >= k)(kv_copy(0, k, 0, mate).wait_recv)

    at(14)
    for d in range(1, half + 1):
        kv_arrival(2 * d)
        there = (post >= d) & ((side == 1) | (d < half))
        move = kv_copy(2 * d, jnp.minimum(2 * d + 1 - 2 * side, reach), half + d, mate)
        kv_moves.append((there, move))
        pl.when(there)(move.start)

    at(15)
    head_dim = kv.shape[2] // 2
    span = (reach + 1) * tok_rows
    at(16)
    position = seq * tok_rows + lax.broadcasted_iota(jnp.int32, (tok_rows, 1), 0)
    begins = jnp.zeros((tok_rows, 1), jnp.int32)
    total_length = jnp.int32(0)
    for k in range(doc_lengths.shape[1]):
        begins = jnp.where(position >= total_length, total_length, begins)
        total_length = total_length + doc_lengths[0, k]
    key_pos = (seq - reach) * tok_rows + lax.broadcasted_iota(jnp.int32, (tok_rows, span), 1)
    allowed = (key_pos >= begins) & (key_pos <= position)
    for k in range(1, reach, 2):
        kv_arrival(k)
    everything = kv[...].reshape(span, 2 * head_dim)
    keys, values = everything[:, :head_dim], everything[:, head_dim:]
    for h in range(query_width // head_dim):
        scores = lax.dot_general(
            queries[:, h * head_dim : (h + 1) * head_dim], keys,
            (((1,), (1,)), ((), ())), preferred_element_type=f32,
        ) * head_dim ** (-0.5)
        scores = jnp.where(allowed, scores, -1e30)
        weights = jnp.exp(scores - jnp.max(scores, axis=-1, keepdims=True))
        totals = jnp.sum(weights, axis=-1, keepdims=True)
        mixed = jnp.dot(weights.astype(bf16), values, preferred_element_type=f32)
        attended[:, h * head_dim : (h + 1) * head_dim] = (mixed / totals).astype(bf16)
    at(17)
    out_relay.flush()
    out_relay.settle()

    n_dev = n_grp * n_seq
    out_width = attn_out.shape[1]
    streamed = out_width % LANES != 0
    ahead = AHEAD if streamed else 0
    out_loads = [
        pltpu.make_async_copy(out_all.at[i], out_v.at[i % AHEAD], out_sem.at[i % AHEAD])
        for i in range(n_dev if streamed else 0)
    ]
    for i in range(ahead):
        out_loads[i].start()
    stores = []
    for c in range(n_seq):
        for j in range(n_grp):
            i = c * n_grp + j
            if streamed:
                out_loads[i].wait()
            weight = out_v[i % AHEAD] if streamed else out_all[i]
            update = jnp.dot(attended[...], weight, preferred_element_type=f32)
            if streamed and i + AHEAD < n_dev:
                out_loads[i + AHEAD].start()
            columns = slice(j * out_width, (j + 1) * out_width)
            held = chunk(c)
            held[:, columns] = (held[:, columns].astype(f32) + update).astype(bf16)
        stores.append(
            pltpu.make_async_copy(chunk(c), result.at[:, chunk_columns(c)], result_sem.at[c])
        )
        stores[-1].start()
    for store in stores:
        store.wait()
    first.end()
    second.end()
    for move in table_moves:
        move.wait_send()
    for there, move in kv_moves:
        pl.when(there)(move.wait_send)
    relay.end()
    out_relay.end()


VMEM = pl.BlockSpec(memory_space=pltpu.VMEM)
SMEM = pl.BlockSpec(memory_space=pltpu.SMEM)
ANY = pl.BlockSpec(memory_space=pl.ANY)


def on_device(
    patches, piece_ids, vit_gain, vit_qkv, vit_out, merge_gain, merge_up, merge_down, dest,
    tokens, image_index, doc_lengths, attn_gain, attn_qkv, attn_out,
):
    rows, features = patches.shape
    n_seq, n_grp = lax.axis_size("seq"), lax.axis_size("grp")
    n_dev = n_seq * n_grp
    own = rows // 4
    capacity = own // (n_seq // 2)
    slots = n_seq * capacity
    reach = n_seq // 2
    line = n_seq // 2
    bf16, f32 = jnp.bfloat16, jnp.float32
    tok_rows = tokens.shape[0]
    query_width, out_width = attn_out.shape
    kv_width = attn_qkv.shape[1] - query_width
    down_width = merge_down.shape[1]
    dma = pltpu.SemaphoreType.DMA
    streamed = out_width % LANES != 0
    out_all_shape = (n_dev,) + attn_out.shape
    outputs = [jax.ShapeDtypeStruct(tokens.shape, bf16)]
    held = [pltpu.VMEM(out_all_shape, bf16)]
    if streamed:
        outputs.append(jax.ShapeDtypeStruct(out_all_shape, bf16))
        held = []
    results = pl.pallas_call(
        functools.partial(layer_kernel, n_grp, n_seq, capacity, reach),
        out_shape=tuple(outputs),
        in_specs=[VMEM] * 6 + [SMEM] * 2 + [ANY] * 7,
        out_specs=(ANY,) * len(outputs),
        scratch_shapes=held + [
            pltpu.VMEM(vit_qkv.shape, bf16),
            pltpu.VMEM(vit_out.shape, bf16),
            pltpu.VMEM(merge_up.shape, bf16),
            pltpu.VMEM(merge_down.shape, bf16),
            pltpu.VMEM((n_dev,) + attn_qkv.shape, bf16),
            pltpu.VMEM((features // LANES, rows, LANES), f32),
            pltpu.VMEM((n_seq, own, 4 * features + LANES), bf16),
            pltpu.VMEM((n_seq, n_seq * own, merge_up.shape[1]), bf16),
            pltpu.VMEM((n_seq, slots, down_width), bf16),
            pltpu.VMEM((n_seq, slots, down_width), bf16),
            pltpu.VMEM((tok_rows, query_width), bf16),
            pltpu.VMEM((reach + 1, tok_rows, kv_width), bf16),
            pltpu.VMEM((tok_rows, query_width), bf16),
            pltpu.VMEM((AHEAD, query_width if streamed else 16, out_width), bf16),
            dma((6,)), dma((n_seq,)), dma((n_seq,)), dma((AHEAD,)),
            dma((2, line)), dma((2, line)), dma((n_seq,)), dma((n_seq,)),
            dma((n_seq,)), dma((n_seq,)), dma((reach + 2,)), dma((reach + 1,)),
        ] + relay_scratch(n_dev) + relay_scratch(n_dev),
        compiler_params=pltpu.CompilerParams(
            collective_id=0, has_side_effects=True, vmem_limit_bytes=67043328
        ),
    )(
        patches, piece_ids, vit_gain, merge_gain, attn_gain, image_index, dest, doc_lengths,
        vit_qkv, vit_out, merge_up, merge_down, tokens, attn_qkv, attn_out,
    )
    return results[0]


def solution(mesh):
    placed = (
        P(("grp", "seq"), None),
        P(("grp", "seq"), None),
        P(),
        P(),
        P(),
        P(),
        P(None, "seq"),
        P(None, "seq"),
        P(("grp", "seq")),
        P(("grp", "seq"), None),
        P(("grp", "seq")),
        P("grp", None),
        P(),
        P(("grp", "seq"), None),
        P(None, ("grp", "seq")),
    )
    return jax.shard_map(
        on_device, mesh=mesh, in_specs=placed, out_specs=P(("grp", "seq"), None), check_vma=False
    )
```

```python
import functools
import math

import jax
import jax.numpy as jnp
from jax import lax
from jax.experimental import pallas as pl
from jax.experimental.pallas import tpu as pltpu
from jax.sharding import PartitionSpec as P

VHEADS = 16
WIN = 64
LANES = 128
EPSILON = 1e-06
AHEAD = 8
PLAN = {0: ('wsx', 'ra0xc'), 1: ('ro1y', 'ro1xc'), (1, 2): (), 6: ('ra1', 'ro3', 'wsy', 'wsz', 'wsc'), (2, 2): ('ra2',), 10: ('ra3', 'wo1', 'wa0'), 11: ('rb0', 'rb1', 'rb2', 'rb3', 'wo2'), (1, 1): ('ro1z',), (1, 3): ('ro2',), 12: ('wa1', 'wo3'), 14: ('wa2',), 15: ('wa3',), 16: ('wb0', 'wb1'), 17: ('wb2', 'wb3')}
MESH = pl.DeviceIdType.MESH


def rms_scale(inputs, gain):
    mean_square = jnp.mean(inputs * inputs, axis=-1, keepdims=True)
    return inputs * lax.rsqrt(mean_square + EPSILON) * gain


def whole_part(values, divisor):
    return jnp.floor((values + 0.5) / divisor)


def greet(n_seq, pairs):
    grp, seq = lax.axis_index("grp"), lax.axis_index("seq")
    barrier = pltpu.get_barrier_semaphore()
    for k in range(1, n_seq):
        pl.semaphore_signal(
            barrier, inc=1, device_id=(grp, lax.rem(seq + k, n_seq)), device_id_type=MESH
        )
    for other in pairs:
        pl.semaphore_signal(barrier, inc=1, device_id=(other, seq), device_id_type=MESH)
    pl.semaphore_wait(barrier, n_seq - 1 + len(pairs))


def flip(index, bit):
    return index + bit - 2 * bit * lax.rem(index // bit, 2)


def opposite(flag):
    return (not flag) if isinstance(flag, bool) else jnp.logical_not(flag)


def either(left, right):
    if left is True or right is True:
        return True
    if left is False:
        return right
    return left if right is False else left | right


def both(left, right):
    if left is False or right is False:
        return False
    if left is True:
        return right
    return left if right is True else left & right


class Relay:
    def __init__(self, n_seq, shard, full, first, plane, local_sem, recv_sem, send_sem):
        self.n_seq, self.shard, self.full = n_seq, shard, full
        self.local_sem, self.recv_sem, self.send_sem = local_sem, recv_sem, send_sem
        self.line = n_seq // 2
        self.grp, self.seq = lax.axis_index("grp"), lax.axis_index("seq")
        self.plane, self.first, self.done = plane, first, []
        self.place, self.side = self.seq // 2, lax.rem(self.seq, 2)
        far = flip(self.grp, 2)
        self.far = far
        across = flip(self.seq, 1)
        self.a_dev = (jnp.where(first, far, self.grp), jnp.where(first, self.seq, across))
        self.b_dev = (jnp.where(first, self.grp, far), jnp.where(first, across, self.seq))
        self.ab_dev = (far, across)
        self.core_dev = (flip(self.grp, 1), self.seq)

    def slot(self, base, place):
        return base[0] * self.n_seq + 2 * place + lax.rem(base[1], 2)

    def copy(self, slot, way, device, own=False):
        return pltpu.make_async_remote_copy(
            src_ref=self.shard if own else self.full.at[slot],
            dst_ref=self.full.at[slot],
            send_sem=self.send_sem.at[way, slot],
            recv_sem=self.recv_sem.at[slot],
            device_id=device,
            device_id_type=MESH,
        )

    def up(self):
        return (self.grp, jnp.minimum(self.seq + 2, self.n_seq - 2 + self.side))

    def down(self):
        return (self.grp, jnp.maximum(self.seq - 2, self.side))

    def me(self):
        return (self.grp, self.seq)

    def launch(self, kind):
        slot = self.slot(self.me(), self.place)
        if kind == "c":
            pltpu.make_async_copy(self.shard, self.full.at[slot], self.local_sem).start()
            self.copy(slot, 4, self.core_dev, True).start()
        elif kind == "z":

            @pl.when(self.place + 1 < self.line)
            def _():
                self.copy(slot, 0, self.up(), True).start()

            @pl.when(self.place > 0)
            def _():
                self.copy(slot, 1, self.down(), True).start()

        else:
            way, device = self.side_way(kind)
            self.copy(slot, way, device, True).start()

    def spots(self, distance):
        low, high = self.place - distance, self.place + distance
        if distance == 0:
            return [(self.place, None, None)]
        return [(low, low >= 0, True), (high, high < self.line, False)]

    def pass_on(self, slot, way, device, guard, finish):
        def act():
            move = self.copy(slot, way, device)
            move.wait_send() if finish else move.start()

        if guard is True:
            act()
        elif guard is not False:
            pl.when(guard)(act)

    def visit(self, base, distance, ways, finish):
        for place, there, upward in self.spots(distance):

            def act(place=place, upward=upward):
                slot = self.slot(base, place)
                for kind, guard in ways:
                    if kind == "r":
                        self.copy(slot, 4, self.core_dev).wait_recv()
                    elif kind == "z":
                        if upward is not False:
                            room = both(guard, self.place + 1 < self.line)
                            self.pass_on(slot, 0, self.up(), room, finish)
                        if upward is not True:
                            room = both(guard, self.place > 0)
                            self.pass_on(slot, 1, self.down(), room, finish)
                    elif kind == "c":
                        self.pass_on(slot, 4, self.core_dev, guard, finish)
                    else:
                        self.pass_on(slot, *self.side_way(kind), guard, finish)

            if there is None:
                act()
            else:
                pl.when(there)(act)

    def side_way(self, kind):
        a_way = self.first if kind == "x" else opposite(self.first)
        device = (self.far, self.seq) if kind == "x" else (self.grp, flip(self.seq, 1))
        return jnp.where(a_way, 2, 3), device

    def forward(self, kind, distance, ways, finish=False):
        later = opposite(self.plane)
        guards = {
            "o": {
                "x": either(opposite(self.first), later), "y": either(self.first, later),
                "z": True, "c": True,
            },
            "a": {"x": opposite(self.first), "y": self.first, "z": self.plane, "c": True},
            "b": {"c": True},
        }[kind]
        chosen = [("r", True)] if "r" in ways else []
        chosen += [(way, guards[way]) for way in ways if way in guards]
        bases = {"o": [self.me()], "a": [self.a_dev], "b": [self.b_dev, self.ab_dev]}[kind]
        for base in bases:
            self.visit(base, distance, chosen, finish)

    def run(self, name):
        if name[0] == "s":
            if name not in self.done:
                self.launch(name[1])
            self.done.append(name)
            return
        kind, distance = name[0], int(name[1])
        self.run_ways(kind, distance, name[2:] or "xyzc")

    def run_ways(self, kind, distance, ways):
        if distance >= self.line:
            return
        ways = [way for way in "r" + ways if (kind, distance, way) not in self.done]
        self.done += [(kind, distance, way) for way in ways]
        if ways:
            self.forward(kind, distance, ways)

    def flush(self):
        for kind in "xyzc":
            self.run("s" + kind)
        for kind in "oab":
            for distance in range(kind == "o", self.line):
                self.run_ways(kind, distance, "xyzc")

    def end(self):
        slot = self.slot(self.me(), self.place)

        @pl.when(self.place + 1 < self.line)
        def _():
            self.copy(slot, 0, self.up(), True).wait_send()

        @pl.when(self.place > 0)
        def _():
            self.copy(slot, 1, self.down(), True).wait_send()

        self.copy(slot, 2, self.a_dev, True).wait_send()
        self.copy(slot, 3, self.b_dev, True).wait_send()
        self.copy(slot, 4, self.core_dev, True).wait_send()
        for kind in "oab":
            for distance in range(kind == "o", self.line):
                self.forward(kind, distance, "xyzc", True)

    def settle(self):
        slot = self.slot(self.me(), self.place)
        pltpu.make_async_copy(self.shard, self.full.at[slot], self.local_sem).wait()
        partner = self.core_dev[0]
        for place in range(self.line):
            for base in (
                (partner, self.seq), (partner, flip(self.seq, 1)),
                (flip(partner, 2), self.seq), (flip(partner, 2), flip(self.seq, 1)),
            ):
                slot = self.slot(base, place)
                self.copy(slot, 4, self.core_dev).wait_recv()


class Gather:
    def __init__(self, n_seq, buf, send_sem, recv_sem):
        self.buf, self.send_sem, self.recv_sem = buf, send_sem, recv_sem
        self.line = n_seq // 2
        self.grp, self.seq = lax.axis_index("grp"), lax.axis_index("seq")
        self.place, self.side = self.seq // 2, lax.rem(self.seq, 2)

    def copy(self, slot, way, place, device):
        return pltpu.make_async_remote_copy(
            src_ref=self.buf.at[slot],
            dst_ref=self.buf.at[slot],
            send_sem=self.send_sem.at[way, place],
            recv_sem=self.recv_sem.at[slot],
            device_id=device,
            device_id_type=MESH,
        )

    def across(self):
        return (self.grp, flip(self.seq, 1))

    def begin(self, finish=False):
        for step in (1, -1):
            to = self.place + step

            @pl.when((to >= 0) & (to < self.line))
            def _():
                move = self.copy(self.seq, 1 + step, self.place, (self.grp, self.seq + 2 * step))
                move.wait_send() if finish else move.start()

        move = self.copy(self.seq, 1, self.place, self.across())
        move.wait_send() if finish else move.start()

    def forward(self, distance, finish=False):
        low, high = self.place - distance, self.place + distance
        for place, there, step in ((low, low >= 0, 1), (high, high < self.line, -1)):

            @pl.when(there)
            def _():
                slot = 2 * place + self.side
                to = self.place + step
                move = self.copy(slot, 1, place, self.across())
                if not finish:
                    move.wait_recv()

                @pl.when((to >= 0) & (to < self.line))
                def _():
                    onward = self.copy(slot, 1 + step, place, (self.grp, self.seq + 2 * step))
                    onward.wait_send() if finish else onward.start()

                move.wait_send() if finish else move.start()

    def settle(self):
        for place in range(self.line):
            slot = 2 * place + 1 - self.side
            self.copy(slot, 1, place, self.across()).wait_recv()

    def end(self):
        self.begin(True)
        for distance in range(1, self.line):
            self.forward(distance, True)


def relay_scratch(n_dev):
    return [
        pltpu.SemaphoreType.DMA,
        pltpu.SemaphoreType.DMA((n_dev,)),
        pltpu.SemaphoreType.DMA((5, n_dev)),
    ]


def swap(n_seq, send_of, land_of, send_sem, recv_sem):
    grp, seq = lax.axis_index("grp"), lax.axis_index("seq")
    moves = []
    for k in range(1, n_seq):
        to = lax.rem(seq + k, n_seq)
        moves.append(
            pltpu.make_async_remote_copy(
                src_ref=send_of(to),
                dst_ref=land_of(seq),
                send_sem=send_sem.at[k],
                recv_sem=recv_sem.at[k],
                device_id=(grp, to),
                device_id_type=MESH,
            )
        )
    for move in moves:
        move.start()
    return moves


def row_codes(dest, rows, capacity):
    order = lax.broadcasted_iota(jnp.int32, (rows, LANES), 0)
    target = jnp.zeros((rows, LANES), jnp.int32)
    for r in range(rows):
        target = jnp.where(order == r, dest[r], target)
    earlier = jnp.zeros((rows, LANES), jnp.int32)
    for r in range(rows):
        earlier = earlier + jnp.where((target == dest[r]) & (order > r), 1, 0)
    return (target * capacity + earlier).astype(jnp.float32)


def window_attention(projected, pieces, features):
    queries, keys, values = projected
    rows = queries.shape[0]
    head_dim = features // VHEADS
    together = LANES // math.gcd(LANES, head_dim)
    width = together * head_dim
    wide = jnp.broadcast_to(pieces.astype(jnp.float32), (rows, rows))
    allowed = wide == jnp.transpose(wide)
    lane = lax.broadcasted_iota(jnp.int32, (rows, width), 1)
    inside = [(lane >= h * head_dim) & (lane < (h + 1) * head_dim) for h in range(together)]
    parts = []
    for start in range(0, features, width):
        q = queries[:, start : start + width]
        stacked = jnp.concatenate(
            [jnp.where(inside[h], q, 0.0).astype(jnp.bfloat16) for h in range(together)], axis=0
        )
        scores = lax.dot_general(
            stacked, keys[:, start : start + width], (((1,), (1,)), ((), ())),
            preferred_element_type=jnp.float32,
        ) * head_dim ** (-0.5)
        scores = jnp.where(allowed[None], scores.reshape(together, rows, rows), -1e30)
        weights = jnp.exp(scores - jnp.max(scores, axis=-1, keepdims=True))
        totals = jnp.sum(weights, axis=-1, keepdims=True)
        mixed = jnp.dot(
            weights.reshape(together * rows, rows).astype(jnp.bfloat16),
            values[:, start : start + width],
            preferred_element_type=jnp.float32,
        )
        top = jnp.zeros((rows, width), jnp.float32)
        low = jnp.ones((rows, width), jnp.float32)
        for h in range(together):
            top = jnp.where(inside[h], mixed[h * rows : (h + 1) * rows], top)
            low = jnp.where(inside[h], totals[h], low)
        parts.append((top / low).astype(jnp.bfloat16))
    return jnp.concatenate(parts, axis=1)


def layer_kernel(
    n_grp, n_seq, capacity, reach,
    patches, pieces, vit_gain, merge_gain, attn_gain, image_index, dest, doc_lengths,
    vit_qkv, vit_out, merge_up, merge_down, tokens, attn_qkv, attn_out,
    result, out_all,
    wide_v, vit_out_v, up_v, down_v, qkv_all, normed_s, gathered, hidden, stage, landed,
    queries, kv, attended, out_v,
    load_sem, token_sem, result_sem, out_sem, gather_send, hidden_send, gather_recv, hidden_recv,
    table_send, table_recv, kv_send, kv_recv, *relay_sems,
):
    grp, seq = lax.axis_index("grp"), lax.axis_index("seq")
    bf16, f32 = jnp.bfloat16, jnp.float32
    rows, features = patches.shape
    tok_rows = tokens.shape[0]
    slots = n_seq * capacity
    part = features
    vit_loads = [
        pltpu.make_async_copy(
            vit_qkv.at[:, pl.ds(i * part, part)], wide_v.at[:, pl.ds(i * part, part)],
            load_sem.at[i],
        )
        for i in range(3)
    ]
    vit_out_load = pltpu.make_async_copy(vit_out, vit_out_v, load_sem.at[3])
    up_load = pltpu.make_async_copy(merge_up, up_v, load_sem.at[4])
    down_load = pltpu.make_async_copy(merge_down, down_v, load_sem.at[5])
    for load in vit_loads + [vit_out_load]:
        load.start()
    greet(n_seq, (flip(grp, 1), flip(grp, 2)))
    core = lax.rem(grp, 2)
    relay = Relay(n_seq, attn_qkv, qkv_all, False, False, *relay_sems[:3])
    for kind in "xyzc":
        relay.run("s" + kind)
    out_relay = Relay(n_seq, attn_out, out_all, core == 0, core == 1, *relay_sems[3:])

    def at(point):
        for name in PLAN.get(point, ()):
            (out_relay if name[0] == "w" else relay).run(name[1:])


    chunk_width = merge_down.shape[1]
    per_row = vit_qkv.shape[1] // chunk_width

    def chunk(c):
        return wide_v.at[
            pl.ds((c // per_row) * tok_rows, tok_rows),
            pl.ds((c % per_row) * chunk_width, chunk_width),
        ]

    def chunk_columns(c):
        return pl.ds(c * chunk_width, chunk_width)

    residual = patches[...].astype(f32)
    normed = rms_scale(residual, vit_gain[...].reshape(1, features)).astype(bf16)
    projected = []
    for i in range(3):
        vit_loads[i].wait()
        projected.append(
            jnp.dot(
                normed, wide_v[:, i * part : (i + 1) * part], preferred_element_type=f32
            ).astype(bf16)
        )
    up_load.start()
    down_load.start()
    token_loads = [
        pltpu.make_async_copy(tokens.at[:, chunk_columns(c)], chunk(c), token_sem.at[c])
        for c in range(n_seq)
    ]
    mixture = window_attention(projected, pieces[...], features)
    at(0)
    vit_out_load.wait()
    residual = residual + jnp.dot(mixture, vit_out_v[...], preferred_element_type=f32)
    merged_in = rms_scale(residual, merge_gain[...].reshape(1, features))
    own = rows // 4
    pieces_of = features // LANES
    for j in range(pieces_of):
        normed_s[j] = merged_in[:, j * LANES : (j + 1) * LANES]
    for quarter in range(4):
        for j in range(pieces_of):
            start = quarter * features + j * LANES
            gathered[seq, :, start : start + LANES] = normed_s[
                j, pl.ds(quarter, own, stride=4), :
            ].astype(bf16)
    gathered[seq, :, 4 * features :] = row_codes(dest, own, capacity).astype(bf16)
    first = Gather(n_seq, gathered, gather_send, gather_recv)
    first.begin()
    at(1)
    for load in token_loads:
        load.start()
    line = n_seq // 2
    for distance in range(1, line):
        first.forward(distance)
        at((1, distance))
    first.settle()
    at(5)
    up_load.wait()

    all_rows = n_seq * own
    entry = gathered[:, :, : 4 * features].reshape(all_rows, 4 * features)
    pre = jnp.dot(entry, up_v[...], preferred_element_type=f32)
    hidden[seq] = (0.5 * pre * (1.0 + lax.erf(pre * 0.5**0.5))).astype(bf16)
    second = Gather(n_seq, hidden, hidden_send, hidden_recv)
    second.begin()
    at(6)

    codes = gathered[:, :, 4 * features :].reshape(all_rows, LANES).astype(f32)[:, :1]
    row = lax.broadcasted_iota(jnp.int32, (all_rows, 1), 0).astype(f32)
    keys = codes + whole_part(row, own) * (n_seq * capacity)
    column = lax.broadcasted_iota(jnp.int32, (1, n_seq * slots), 1).astype(f32)
    target = whole_part(column, slots)
    place = column - target * slots
    source = whole_part(place, capacity)
    want = source * (n_seq * capacity) + target * capacity + place - source * capacity
    select = jnp.transpose(jnp.where(keys == want, 1.0, 0.0)).astype(bf16)

    for distance in range(1, line):
        second.forward(distance)
        at((2, distance))
    down_load.wait()
    part_width = hidden.shape[2]

    def term(index):
        start = pl.multiple_of(index * part_width, 32)
        return jnp.dot(
            hidden[index], down_v[pl.ds(start, part_width), :], preferred_element_type=f32
        )

    side = lax.rem(seq, 2)
    total = term(side)
    for p in range(1, line):
        total = total + term(2 * p + side)
    at(10)
    second.settle()
    for p in range(line):
        total = total + term(2 * p + 1 - side)
    outgoing = jnp.dot(select, total.astype(bf16), preferred_element_type=f32).astype(bf16)
    stage[...] = outgoing.reshape(stage.shape)
    landed[seq] = stage[seq]
    table_moves = swap(
        n_seq, lambda to: stage.at[to], lambda me: landed.at[me], table_send, table_recv
    )
    at(11)
    slot = lax.broadcasted_iota(jnp.int32, (slots, tok_rows), 0)
    picked = jnp.where(slot == image_index[...].reshape(1, tok_rows), 1.0, 0.0)
    picker = jnp.transpose(picked)
    pictured = jnp.sum(picker, axis=1, keepdims=True) > 0.5
    picker = picker.astype(bf16)
    square = jnp.zeros((tok_rows, 1), f32)
    for load in token_loads:
        load.wait()
    for k in range(n_seq):
        if k:
            table_moves[k - 1].wait_recv()
        c = lax.rem(seq - k + n_seq, n_seq)
        rows_at = pl.multiple_of((c // per_row) * tok_rows, tok_rows)
        columns_at = pl.multiple_of((c % per_row) * chunk_width, chunk_width)
        held = wide_v.at[pl.ds(rows_at, tok_rows), pl.ds(columns_at, chunk_width)]
        image = jnp.dot(picker, landed[c], preferred_element_type=f32)
        layer_in = jnp.where(pictured, image, held[...].astype(f32))
        held[...] = layer_in.astype(bf16)
        square = square + jnp.sum(layer_in * layer_in, axis=1, keepdims=True)
    at(12)
    scale = lax.rsqrt(square / (n_seq * chunk_width) + EPSILON)
    at(13)
    relay.flush()
    relay.settle()
    shard_rows, qkv_width = attn_qkv.shape
    attn_projected = jnp.zeros((tok_rows, qkv_width), f32)
    for c in range(n_seq):
        gain = attn_gain[pl.ds(c * chunk_width, chunk_width)].reshape(1, chunk_width)
        tokens_in = (chunk(c)[...].astype(f32) * scale * gain).astype(bf16)
        weight = qkv_all[c * n_grp : (c + 1) * n_grp].reshape(n_grp * shard_rows, qkv_width)
        attn_projected = attn_projected + jnp.dot(tokens_in, weight, preferred_element_type=f32)
    query_width = attn_out.shape[0]
    queries[...] = attn_projected[:, :query_width].astype(bf16)
    kv[reach] = attn_projected[:, query_width:].astype(bf16)
    half = reach // 2
    post = seq // 2

    def kv_copy(k_from, k_to, way, device):
        return pltpu.make_async_remote_copy(
            src_ref=kv.at[reach - k_from],
            dst_ref=kv.at[reach - k_to],
            send_sem=kv_send.at[way],
            recv_sem=kv_recv.at[k_to],
            device_id=device,
            device_id_type=MESH,
        )

    mate = (grp, flip(seq, 1))
    kv_moves = [(side == 0, kv_copy(0, 1, 0, mate))]
    for d in range(1, half + 1):
        ahead = (grp, jnp.minimum(seq + 2 * d, n_seq - 1))
        kv_moves.append((post + d < line, kv_copy(0, 2 * d, d, ahead)))
    for there, move in kv_moves:
        pl.when(there)(move.start)
    for k in range(1, reach + 1):

        @pl.when(seq < k)
        def _():
            kv[reach - k] = jnp.zeros(kv.shape[1:], bf16)

    def kv_arrival(k):
        pl.when(seq >= k)(kv_copy(0, k, 0, mate).wait_recv)

    at(14)
    for d in range(1, half + 1):
        kv_arrival(2 * d)
        there = (post >= d) & ((side == 1) | (d < half))
        move = kv_copy(2 * d, jnp.minimum(2 * d + 1 - 2 * side, reach), half + d, mate)
        kv_moves.append((there, move))
        pl.when(there)(move.start)

    at(15)
    head_dim = kv.shape[2] // 2
    span = (reach + 1) * tok_rows
    at(16)
    position = seq * tok_rows + lax.broadcasted_iota(jnp.int32, (tok_rows, 1), 0)
    begins = jnp.zeros((tok_rows, 1), jnp.int32)
    total_length = jnp.int32(0)
    for k in range(doc_lengths.shape[1]):
        begins = jnp.where(position >= total_length, total_length, begins)
        total_length = total_length + doc_lengths[0, k]
    key_pos = (seq - reach) * tok_rows + lax.broadcasted_iota(jnp.int32, (tok_rows, span), 1)
    allowed = (key_pos >= begins) & (key_pos <= position)
    for k in range(1, reach, 2):
        kv_arrival(k)
    everything = kv[...].reshape(span, 2 * head_dim)
    keys, values = everything[:, :head_dim], everything[:, head_dim:]
    for h in range(query_width // head_dim):
        scores = lax.dot_general(
            queries[:, h * head_dim : (h + 1) * head_dim], keys,
            (((1,), (1,)), ((), ())), preferred_element_type=f32,
        ) * head_dim ** (-0.5)
        scores = jnp.where(allowed, scores, -1e30)
        weights = jnp.exp(scores - jnp.max(scores, axis=-1, keepdims=True))
        totals = jnp.sum(weights, axis=-1, keepdims=True)
        mixed = jnp.dot(weights.astype(bf16), values, preferred_element_type=f32)
        attended[:, h * head_dim : (h + 1) * head_dim] = (mixed / totals).astype(bf16)
    at(17)
    out_relay.flush()
    out_relay.settle()

    n_dev = n_grp * n_seq
    out_width = attn_out.shape[1]
    streamed = out_width % LANES != 0
    ahead = AHEAD if streamed else 0
    out_loads = [
        pltpu.make_async_copy(out_all.at[i], out_v.at[i % AHEAD], out_sem.at[i % AHEAD])
        for i in range(n_dev if streamed else 0)
    ]
    for i in range(ahead):
        out_loads[i].start()
    stores = []
    for c in range(n_seq):
        for j in range(n_grp):
            i = c * n_grp + j
            if streamed:
                out_loads[i].wait()
            weight = out_v[i % AHEAD] if streamed else out_all[i]
            update = jnp.dot(attended[...], weight, preferred_element_type=f32)
            if streamed and i + AHEAD < n_dev:
                out_loads[i + AHEAD].start()
            columns = slice(j * out_width, (j + 1) * out_width)
            held = chunk(c)
            held[:, columns] = (held[:, columns].astype(f32) + update).astype(bf16)
        stores.append(
            pltpu.make_async_copy(chunk(c), result.at[:, chunk_columns(c)], result_sem.at[c])
        )
        stores[-1].start()
    for store in stores:
        store.wait()
    first.end()
    second.end()
    for move in table_moves:
        move.wait_send()
    for there, move in kv_moves:
        pl.when(there)(move.wait_send)
    relay.end()
    out_relay.end()


VMEM = pl.BlockSpec(memory_space=pltpu.VMEM)
SMEM = pl.BlockSpec(memory_space=pltpu.SMEM)
ANY = pl.BlockSpec(memory_space=pl.ANY)


def on_device(
    patches, piece_ids, vit_gain, vit_qkv, vit_out, merge_gain, merge_up, merge_down, dest,
    tokens, image_index, doc_lengths, attn_gain, attn_qkv, attn_out,
):
    rows, features = patches.shape
    n_seq, n_grp = lax.axis_size("seq"), lax.axis_size("grp")
    n_dev = n_seq * n_grp
    own = rows // 4
    capacity = own // (n_seq // 2)
    slots = n_seq * capacity
    reach = n_seq // 2
    line = n_seq // 2
    bf16, f32 = jnp.bfloat16, jnp.float32
    tok_rows = tokens.shape[0]
    query_width, out_width = attn_out.shape
    kv_width = attn_qkv.shape[1] - query_width
    down_width = merge_down.shape[1]
    dma = pltpu.SemaphoreType.DMA
    streamed = out_width % LANES != 0
    out_all_shape = (n_dev,) + attn_out.shape
    outputs = [jax.ShapeDtypeStruct(tokens.shape, bf16)]
    held = [pltpu.VMEM(out_all_shape, bf16)]
    if streamed:
        outputs.append(jax.ShapeDtypeStruct(out_all_shape, bf16))
        held = []
    results = pl.pallas_call(
        functools.partial(layer_kernel, n_grp, n_seq, capacity, reach),
        out_shape=tuple(outputs),
        in_specs=[VMEM] * 6 + [SMEM] * 2 + [ANY] * 7,
        out_specs=(ANY,) * len(outputs),
        scratch_shapes=held + [
            pltpu.VMEM(vit_qkv.shape, bf16),
            pltpu.VMEM(vit_out.shape, bf16),
            pltpu.VMEM(merge_up.shape, bf16),
            pltpu.VMEM(merge_down.shape, bf16),
            pltpu.VMEM((n_dev,) + attn_qkv.shape, bf16),
            pltpu.VMEM((features // LANES, rows, LANES), f32),
            pltpu.VMEM((n_seq, own, 4 * features + LANES), bf16),
            pltpu.VMEM((n_seq, n_seq * own, merge_up.shape[1]), bf16),
            pltpu.VMEM((n_seq, slots, down_width), bf16),
            pltpu.VMEM((n_seq, slots, down_width), bf16),
            pltpu.VMEM((tok_rows, query_width), bf16),
            pltpu.VMEM((reach + 1, tok_rows, kv_width), bf16),
            pltpu.VMEM((tok_rows, query_width), bf16),
            pltpu.VMEM((AHEAD, query_width if streamed else 16, out_width), bf16),
            dma((6,)), dma((n_seq,)), dma((n_seq,)), dma((AHEAD,)),
            dma((3, line)), dma((3, line)), dma((n_seq,)), dma((n_seq,)),
            dma((n_seq,)), dma((n_seq,)), dma((reach + 2,)), dma((reach + 1,)),
        ] + relay_scratch(n_dev) + relay_scratch(n_dev),
        compiler_params=pltpu.CompilerParams(
            collective_id=0, has_side_effects=True, vmem_limit_bytes=67043328
        ),
    )(
        patches, piece_ids, vit_gain, merge_gain, attn_gain, image_index, dest, doc_lengths,
        vit_qkv, vit_out, merge_up, merge_down, tokens, attn_qkv, attn_out,
    )
    return results[0]


def solution(mesh):
    placed = (
        P(("grp", "seq"), None),
        P(("grp", "seq"), None),
        P(),
        P(),
        P(),
        P(),
        P(None, "seq"),
        P(None, "seq"),
        P(("grp", "seq")),
        P(("grp", "seq"), None),
        P(("grp", "seq")),
        P("grp", None),
        P(),
        P(("grp", "seq"), None),
        P(None, ("grp", "seq")),
    )
    return jax.shard_map(
        on_device, mesh=mesh, in_specs=placed, out_specs=P(("grp", "seq"), None), check_vma=False
    )
```

```python
import functools
import math

import jax
import jax.numpy as jnp
from jax import lax
from jax.experimental import pallas as pl
from jax.experimental.pallas import tpu as pltpu
from jax.sharding import PartitionSpec as P

VHEADS = 16
WIN = 64
LANES = 128
EPSILON = 1e-06
AHEAD = 8
PLAN = {0: ('ra0xc',), 1: ('ro1y', 'ro1xc', 'wsx'), (1, 2): (), 6: ('ra1', 'ro3', 'wsy', 'wsz', 'wsc'), (2, 2): ('ra2',), 10: ('ra3', 'wo1', 'wa0'), 11: ('rb0', 'rb1', 'rb2', 'rb3', 'wo2'), (1, 1): ('ro1z',), (1, 3): ('ro2',), 12: ('wa1', 'wo3'), 14: ('wa2',), 15: ('wa3',), 16: ('wb0', 'wb1'), 17: ('wb2', 'wb3')}
MESH = pl.DeviceIdType.MESH


def rms_scale(inputs, gain):
    mean_square = jnp.mean(inputs * inputs, axis=-1, keepdims=True)
    return inputs * lax.rsqrt(mean_square + EPSILON) * gain


def whole_part(values, divisor):
    return jnp.floor((values + 0.5) / divisor)


def greet(n_seq, pairs):
    grp, seq = lax.axis_index("grp"), lax.axis_index("seq")
    barrier = pltpu.get_barrier_semaphore()
    for k in range(1, n_seq):
        pl.semaphore_signal(
            barrier, inc=1, device_id=(grp, lax.rem(seq + k, n_seq)), device_id_type=MESH
        )
    for other in pairs:
        pl.semaphore_signal(barrier, inc=1, device_id=(other, seq), device_id_type=MESH)
    pl.semaphore_wait(barrier, n_seq - 1 + len(pairs))


def flip(index, bit):
    return index + bit - 2 * bit * lax.rem(index // bit, 2)


def opposite(flag):
    return (not flag) if isinstance(flag, bool) else jnp.logical_not(flag)


def either(left, right):
    if left is True or right is True:
        return True
    if left is False:
        return right
    return left if right is False else left | right


def both(left, right):
    if left is False or right is False:
        return False
    if left is True:
        return right
    return left if right is True else left & right


class Relay:
    def __init__(self, n_seq, shard, full, first, plane, local_sem, recv_sem, send_sem):
        self.n_seq, self.shard, self.full = n_seq, shard, full
        self.local_sem, self.recv_sem, self.send_sem = local_sem, recv_sem, send_sem
        self.line = n_seq // 2
        self.grp, self.seq = lax.axis_index("grp"), lax.axis_index("seq")
        self.plane, self.first, self.done = plane, first, []
        self.place, self.side = self.seq // 2, lax.rem(self.seq, 2)
        far = flip(self.grp, 2)
        self.far = far
        across = flip(self.seq, 1)
        self.a_dev = (jnp.where(first, far, self.grp), jnp.where(first, self.seq, across))
        self.b_dev = (jnp.where(first, self.grp, far), jnp.where(first, across, self.seq))
        self.ab_dev = (far, across)
        self.core_dev = (flip(self.grp, 1), self.seq)

    def slot(self, base, place):
        return base[0] * self.n_seq + 2 * place + lax.rem(base[1], 2)

    def copy(self, slot, way, device, own=False):
        return pltpu.make_async_remote_copy(
            src_ref=self.shard if own else self.full.at[slot],
            dst_ref=self.full.at[slot],
            send_sem=self.send_sem.at[way, slot],
            recv_sem=self.recv_sem.at[slot],
            device_id=device,
            device_id_type=MESH,
        )

    def up(self):
        return (self.grp, jnp.minimum(self.seq + 2, self.n_seq - 2 + self.side))

    def down(self):
        return (self.grp, jnp.maximum(self.seq - 2, self.side))

    def me(self):
        return (self.grp, self.seq)

    def launch(self, kind):
        slot = self.slot(self.me(), self.place)
        if kind == "c":
            pltpu.make_async_copy(self.shard, self.full.at[slot], self.local_sem).start()
            self.copy(slot, 4, self.core_dev, True).start()
        elif kind == "z":

            @pl.when(self.place + 1 < self.line)
            def _():
                self.copy(slot, 0, self.up(), True).start()

            @pl.when(self.place > 0)
            def _():
                self.copy(slot, 1, self.down(), True).start()

        else:
            way, device = self.side_way(kind)
            self.copy(slot, way, device, True).start()

    def spots(self, distance):
        low, high = self.place - distance, self.place + distance
        if distance == 0:
            return [(self.place, None, None)]
        return [(low, low >= 0, True), (high, high < self.line, False)]

    def pass_on(self, slot, way, device, guard, finish):
        def act():
            move = self.copy(slot, way, device)
            move.wait_send() if finish else move.start()

        if guard is True:
            act()
        elif guard is not False:
            pl.when(guard)(act)

    def visit(self, base, distance, ways, finish):
        for place, there, upward in self.spots(distance):

            def act(place=place, upward=upward):
                slot = self.slot(base, place)
                for kind, guard in ways:
                    if kind == "r":
                        self.copy(slot, 4, self.core_dev).wait_recv()
                    elif kind == "z":
                        if upward is not False:
                            room = both(guard, self.place + 1 < self.line)
                            self.pass_on(slot, 0, self.up(), room, finish)
                        if upward is not True:
                            room = both(guard, self.place > 0)
                            self.pass_on(slot, 1, self.down(), room, finish)
                    elif kind == "c":
                        self.pass_on(slot, 4, self.core_dev, guard, finish)
                    else:
                        self.pass_on(slot, *self.side_way(kind), guard, finish)

            if there is None:
                act()
            else:
                pl.when(there)(act)

    def side_way(self, kind):
        a_way = self.first if kind == "x" else opposite(self.first)
        device = (self.far, self.seq) if kind == "x" else (self.grp, flip(self.seq, 1))
        return jnp.where(a_way, 2, 3), device

    def forward(self, kind, distance, ways, finish=False):
        later = opposite(self.plane)
        guards = {
            "o": {
                "x": either(opposite(self.first), later), "y": either(self.first, later),
                "z": True, "c": True,
            },
            "a": {"x": opposite(self.first), "y": self.first, "z": self.plane, "c": True},
            "b": {"c": True},
        }[kind]
        chosen = [("r", True)] if "r" in ways else []
        chosen += [(way, guards[way]) for way in ways if way in guards]
        bases = {"o": [self.me()], "a": [self.a_dev], "b": [self.b_dev, self.ab_dev]}[kind]
        for base in bases:
            self.visit(base, distance, chosen, finish)

    def run(self, name):
        if name[0] == "s":
            if name not in self.done:
                self.launch(name[1])
            self.done.append(name)
            return
        kind, distance = name[0], int(name[1])
        self.run_ways(kind, distance, name[2:] or "xyzc")

    def run_ways(self, kind, distance, ways):
        if distance >= self.line:
            return
        ways = [way for way in "r" + ways if (kind, distance, way) not in self.done]
        self.done += [(kind, distance, way) for way in ways]
        if ways:
            self.forward(kind, distance, ways)

    def flush(self):
        for kind in "xyzc":
            self.run("s" + kind)
        for kind in "oab":
            for distance in range(kind == "o", self.line):
                self.run_ways(kind, distance, "xyzc")

    def end(self):
        slot = self.slot(self.me(), self.place)

        @pl.when(self.place + 1 < self.line)
        def _():
            self.copy(slot, 0, self.up(), True).wait_send()

        @pl.when(self.place > 0)
        def _():
            self.copy(slot, 1, self.down(), True).wait_send()

        self.copy(slot, 2, self.a_dev, True).wait_send()
        self.copy(slot, 3, self.b_dev, True).wait_send()
        self.copy(slot, 4, self.core_dev, True).wait_send()
        for kind in "oab":
            for distance in range(kind == "o", self.line):
                self.forward(kind, distance, "xyzc", True)

    def settle(self):
        slot = self.slot(self.me(), self.place)
        pltpu.make_async_copy(self.shard, self.full.at[slot], self.local_sem).wait()
        partner = self.core_dev[0]
        for place in range(self.line):
            for base in (
                (partner, self.seq), (partner, flip(self.seq, 1)),
                (flip(partner, 2), self.seq), (flip(partner, 2), flip(self.seq, 1)),
            ):
                slot = self.slot(base, place)
                self.copy(slot, 4, self.core_dev).wait_recv()


class Gather:
    def __init__(self, n_seq, buf, send_sem, recv_sem):
        self.buf, self.send_sem, self.recv_sem = buf, send_sem, recv_sem
        self.line = n_seq // 2
        self.grp, self.seq = lax.axis_index("grp"), lax.axis_index("seq")
        self.place, self.side = self.seq // 2, lax.rem(self.seq, 2)

    def copy(self, slot, way, place, device):
        return pltpu.make_async_remote_copy(
            src_ref=self.buf.at[slot],
            dst_ref=self.buf.at[slot],
            send_sem=self.send_sem.at[way, place],
            recv_sem=self.recv_sem.at[slot],
            device_id=device,
            device_id_type=MESH,
        )

    def across(self):
        return (self.grp, flip(self.seq, 1))

    def begin(self, finish=False):
        for step in (1, -1):
            to = self.place + step

            @pl.when((to >= 0) & (to < self.line))
            def _():
                move = self.copy(self.seq, 1 + step, self.place, (self.grp, self.seq + 2 * step))
                move.wait_send() if finish else move.start()

        move = self.copy(self.seq, 1, self.place, self.across())
        move.wait_send() if finish else move.start()

    def forward(self, distance, finish=False):
        low, high = self.place - distance, self.place + distance
        for place, there, step in ((low, low >= 0, 1), (high, high < self.line, -1)):

            @pl.when(there)
            def _():
                slot = 2 * place + self.side
                to = self.place + step
                move = self.copy(slot, 1, place, self.across())
                if not finish:
                    move.wait_recv()

                @pl.when((to >= 0) & (to < self.line))
                def _():
                    onward = self.copy(slot, 1 + step, place, (self.grp, self.seq + 2 * step))
                    onward.wait_send() if finish else onward.start()

                move.wait_send() if finish else move.start()

    def settle(self):
        for place in range(self.line):
            slot = 2 * place + 1 - self.side
            self.copy(slot, 1, place, self.across()).wait_recv()

    def end(self):
        self.begin(True)
        for distance in range(1, self.line):
            self.forward(distance, True)


def relay_scratch(n_dev):
    return [
        pltpu.SemaphoreType.DMA,
        pltpu.SemaphoreType.DMA((n_dev,)),
        pltpu.SemaphoreType.DMA((5, n_dev)),
    ]


def swap(n_seq, send_of, land_of, send_sem, recv_sem):
    grp, seq = lax.axis_index("grp"), lax.axis_index("seq")
    moves = []
    for k in range(1, n_seq):
        to = lax.rem(seq + k, n_seq)
        moves.append(
            pltpu.make_async_remote_copy(
                src_ref=send_of(to),
                dst_ref=land_of(seq),
                send_sem=send_sem.at[k],
                recv_sem=recv_sem.at[k],
                device_id=(grp, to),
                device_id_type=MESH,
            )
        )
    for move in moves:
        move.start()
    return moves


def row_codes(dest, rows, capacity):
    order = lax.broadcasted_iota(jnp.int32, (rows, LANES), 0)
    target = jnp.zeros((rows, LANES), jnp.int32)
    for r in range(rows):
        target = jnp.where(order == r, dest[r], target)
    earlier = jnp.zeros((rows, LANES), jnp.int32)
    for r in range(rows):
        earlier = earlier + jnp.where((target == dest[r]) & (order > r), 1, 0)
    return (target * capacity + earlier).astype(jnp.float32)


def window_attention(projected, pieces, features):
    queries, keys, values = projected
    rows = queries.shape[0]
    head_dim = features // VHEADS
    together = LANES // math.gcd(LANES, head_dim)
    width = together * head_dim
    wide = jnp.broadcast_to(pieces.astype(jnp.float32), (rows, rows))
    allowed = wide == jnp.transpose(wide)
    lane = lax.broadcasted_iota(jnp.int32, (rows, width), 1)
    inside = [(lane >= h * head_dim) & (lane < (h + 1) * head_dim) for h in range(together)]
    parts = []
    for start in range(0, features, width):
        q = queries[:, start : start + width]
        stacked = jnp.concatenate(
            [jnp.where(inside[h], q, 0.0).astype(jnp.bfloat16) for h in range(together)], axis=0
        )
        scores = lax.dot_general(
            stacked, keys[:, start : start + width], (((1,), (1,)), ((), ())),
            preferred_element_type=jnp.float32,
        ) * head_dim ** (-0.5)
        scores = jnp.where(allowed[None], scores.reshape(together, rows, rows), -1e30)
        weights = jnp.exp(scores - jnp.max(scores, axis=-1, keepdims=True))
        totals = jnp.sum(weights, axis=-1, keepdims=True)
        mixed = jnp.dot(
            weights.reshape(together * rows, rows).astype(jnp.bfloat16),
            values[:, start : start + width],
            preferred_element_type=jnp.float32,
        )
        top = jnp.zeros((rows, width), jnp.float32)
        low = jnp.ones((rows, width), jnp.float32)
        for h in range(together):
            top = jnp.where(inside[h], mixed[h * rows : (h + 1) * rows], top)
            low = jnp.where(inside[h], totals[h], low)
        parts.append((top / low).astype(jnp.bfloat16))
    return jnp.concatenate(parts, axis=1)


def layer_kernel(
    n_grp, n_seq, capacity, reach,
    patches, pieces, vit_gain, merge_gain, attn_gain, image_index, dest, doc_lengths,
    vit_qkv, vit_out, merge_up, merge_down, tokens, attn_qkv, attn_out,
    result, out_all,
    wide_v, vit_out_v, up_v, down_v, qkv_all, normed_s, gathered, hidden, stage, landed,
    queries, kv, attended, out_v,
    load_sem, token_sem, result_sem, out_sem, gather_send, hidden_send, gather_recv, hidden_recv,
    table_send, table_recv, kv_send, kv_recv, *relay_sems,
):
    grp, seq = lax.axis_index("grp"), lax.axis_index("seq")
    bf16, f32 = jnp.bfloat16, jnp.float32
    rows, features = patches.shape
    tok_rows = tokens.shape[0]
    slots = n_seq * capacity
    part = features
    vit_loads = [
        pltpu.make_async_copy(
            vit_qkv.at[:, pl.ds(i * part, part)], wide_v.at[:, pl.ds(i * part, part)],
            load_sem.at[i],
        )
        for i in range(3)
    ]
    vit_out_load = pltpu.make_async_copy(vit_out, vit_out_v, load_sem.at[3])
    up_load = pltpu.make_async_copy(merge_up, up_v, load_sem.at[4])
    down_load = pltpu.make_async_copy(merge_down, down_v, load_sem.at[5])
    for load in vit_loads + [vit_out_load]:
        load.start()
    greet(n_seq, (flip(grp, 1), flip(grp, 2)))
    core = lax.rem(grp, 2)
    relay = Relay(n_seq, attn_qkv, qkv_all, False, False, *relay_sems[:3])
    for kind in "xyzc":
        relay.run("s" + kind)
    out_relay = Relay(n_seq, attn_out, out_all, core == 0, core == 1, *relay_sems[3:])

    def at(point):
        for name in PLAN.get(point, ()):
            (out_relay if name[0] == "w" else relay).run(name[1:])


    chunk_width = merge_down.shape[1]
    per_row = vit_qkv.shape[1] // chunk_width

    def chunk(c):
        return wide_v.at[
            pl.ds((c // per_row) * tok_rows, tok_rows),
            pl.ds((c % per_row) * chunk_width, chunk_width),
        ]

    def chunk_columns(c):
        return pl.ds(c * chunk_width, chunk_width)

    residual = patches[...].astype(f32)
    normed = rms_scale(residual, vit_gain[...].reshape(1, features)).astype(bf16)
    projected = []
    for i in range(3):
        vit_loads[i].wait()
        projected.append(
            jnp.dot(
                normed, wide_v[:, i * part : (i + 1) * part], preferred_element_type=f32
            ).astype(bf16)
        )
    up_load.start()
    down_load.start()
    token_loads = [
        pltpu.make_async_copy(tokens.at[:, chunk_columns(c)], chunk(c), token_sem.at[c])
        for c in range(n_seq)
    ]
    mixture = window_attention(projected, pieces[...], features)
    at(0)
    vit_out_load.wait()
    residual = residual + jnp.dot(mixture, vit_out_v[...], preferred_element_type=f32)
    merged_in = rms_scale(residual, merge_gain[...].reshape(1, features))
    own = rows // 4
    pieces_of = features // LANES
    for j in range(pieces_of):
        normed_s[j] = merged_in[:, j * LANES : (j + 1) * LANES]
    for quarter in range(4):
        for j in range(pieces_of):
            start = quarter * features + j * LANES
            gathered[seq, :, start : start + LANES] = normed_s[
                j, pl.ds(quarter, own, stride=4), :
            ].astype(bf16)
    gathered[seq, :, 4 * features :] = row_codes(dest, own, capacity).astype(bf16)
    first = Gather(n_seq, gathered, gather_send, gather_recv)
    first.begin()
    at(1)
    for load in token_loads:
        load.start()
    line = n_seq // 2
    for distance in range(1, line):
        first.forward(distance)
        at((1, distance))
    first.settle()
    at(5)
    up_load.wait()

    all_rows = n_seq * own
    entry = gathered[:, :, : 4 * features].reshape(all_rows, 4 * features)
    pre = jnp.dot(entry, up_v[...], preferred_element_type=f32)
    hidden[seq] = (0.5 * pre * (1.0 + lax.erf(pre * 0.5**0.5))).astype(bf16)
    second = Gather(n_seq, hidden, hidden_send, hidden_recv)
    second.begin()
    at(6)

    codes = gathered[:, :, 4 * features :].reshape(all_rows, LANES).astype(f32)[:, :1]
    row = lax.broadcasted_iota(jnp.int32, (all_rows, 1), 0).astype(f32)
    keys = codes + whole_part(row, own) * (n_seq * capacity)
    column = lax.broadcasted_iota(jnp.int32, (1, n_seq * slots), 1).astype(f32)
    target = whole_part(column, slots)
    place = column - target * slots
    source = whole_part(place, capacity)
    want = source * (n_seq * capacity) + target * capacity + place - source * capacity
    select = jnp.transpose(jnp.where(keys == want, 1.0, 0.0)).astype(bf16)

    for distance in range(1, line):
        second.forward(distance)
        at((2, distance))
    down_load.wait()
    part_width = hidden.shape[2]

    def term(index):
        start = pl.multiple_of(index * part_width, 32)
        return jnp.dot(
            hidden[index], down_v[pl.ds(start, part_width), :], preferred_element_type=f32
        )

    side = lax.rem(seq, 2)
    total = term(side)
    for p in range(1, line):
        total = total + term(2 * p + side)
    at(10)
    second.settle()
    for p in range(line):
        total = total + term(2 * p + 1 - side)
    outgoing = jnp.dot(select, total.astype(bf16), preferred_element_type=f32).astype(bf16)
    stage[...] = outgoing.reshape(stage.shape)
    landed[seq] = stage[seq]
    table_moves = swap(
        n_seq, lambda to: stage.at[to], lambda me: landed.at[me], table_send, table_recv
    )
    at(11)
    slot = lax.broadcasted_iota(jnp.int32, (slots, tok_rows), 0)
    picked = jnp.where(slot == image_index[...].reshape(1, tok_rows), 1.0, 0.0)
    picker = jnp.transpose(picked)
    pictured = jnp.sum(picker, axis=1, keepdims=True) > 0.5
    picker = picker.astype(bf16)
    square = jnp.zeros((tok_rows, 1), f32)
    for load in token_loads:
        load.wait()
    for k in range(n_seq):
        if k:
            table_moves[k - 1].wait_recv()
        c = lax.rem(seq - k + n_seq, n_seq)
        rows_at = pl.multiple_of((c // per_row) * tok_rows, tok_rows)
        columns_at = pl.multiple_of((c % per_row) * chunk_width, chunk_width)
        held = wide_v.at[pl.ds(rows_at, tok_rows), pl.ds(columns_at, chunk_width)]
        image = jnp.dot(picker, landed[c], preferred_element_type=f32)
        layer_in = jnp.where(pictured, image, held[...].astype(f32))
        held[...] = layer_in.astype(bf16)
        square = square + jnp.sum(layer_in * layer_in, axis=1, keepdims=True)
    at(12)
    scale = lax.rsqrt(square / (n_seq * chunk_width) + EPSILON)
    at(13)
    relay.flush()
    relay.settle()
    shard_rows, qkv_width = attn_qkv.shape
    attn_projected = jnp.zeros((tok_rows, qkv_width), f32)
    for c in range(n_seq):
        gain = attn_gain[pl.ds(c * chunk_width, chunk_width)].reshape(1, chunk_width)
        tokens_in = (chunk(c)[...].astype(f32) * scale * gain).astype(bf16)
        weight = qkv_all[c * n_grp : (c + 1) * n_grp].reshape(n_grp * shard_rows, qkv_width)
        attn_projected = attn_projected + jnp.dot(tokens_in, weight, preferred_element_type=f32)
    query_width = attn_out.shape[0]
    queries[...] = attn_projected[:, :query_width].astype(bf16)
    kv[reach] = attn_projected[:, query_width:].astype(bf16)
    half = reach // 2
    post = seq // 2

    def kv_copy(k_from, k_to, way, device):
        return pltpu.make_async_remote_copy(
            src_ref=kv.at[reach - k_from],
            dst_ref=kv.at[reach - k_to],
            send_sem=kv_send.at[way],
            recv_sem=kv_recv.at[k_to],
            device_id=device,
            device_id_type=MESH,
        )

    mate = (grp, flip(seq, 1))
    kv_moves = [(side == 0, kv_copy(0, 1, 0, mate))]
    for d in range(1, half + 1):
        ahead = (grp, jnp.minimum(seq + 2 * d, n_seq - 1))
        kv_moves.append((post + d < line, kv_copy(0, 2 * d, d, ahead)))
    for there, move in kv_moves:
        pl.when(there)(move.start)
    for k in range(1, reach + 1):

        @pl.when(seq < k)
        def _():
            kv[reach - k] = jnp.zeros(kv.shape[1:], bf16)

    def kv_arrival(k):
        pl.when(seq >= k)(kv_copy(0, k, 0, mate).wait_recv)

    at(14)
    for d in range(1, half + 1):
        kv_arrival(2 * d)
        there = (post >= d) & ((side == 1) | (d < half))
        move = kv_copy(2 * d, jnp.minimum(2 * d + 1 - 2 * side, reach), half + d, mate)
        kv_moves.append((there, move))
        pl.when(there)(move.start)

    at(15)
    head_dim = kv.shape[2] // 2
    span = (reach + 1) * tok_rows
    at(16)
    position = seq * tok_rows + lax.broadcasted_iota(jnp.int32, (tok_rows, 1), 0)
    begins = jnp.zeros((tok_rows, 1), jnp.int32)
    total_length = jnp.int32(0)
    for k in range(doc_lengths.shape[1]):
        begins = jnp.where(position >= total_length, total_length, begins)
        total_length = total_length + doc_lengths[0, k]
    key_pos = (seq - reach) * tok_rows + lax.broadcasted_iota(jnp.int32, (tok_rows, span), 1)
    allowed = (key_pos >= begins) & (key_pos <= position)
    for k in range(1, reach, 2):
        kv_arrival(k)
    everything = kv[...].reshape(span, 2 * head_dim)
    keys, values = everything[:, :head_dim], everything[:, head_dim:]
    for h in range(query_width // head_dim):
        scores = lax.dot_general(
            queries[:, h * head_dim : (h + 1) * head_dim], keys,
            (((1,), (1,)), ((), ())), preferred_element_type=f32,
        ) * head_dim ** (-0.5)
        scores = jnp.where(allowed, scores, -1e30)
        weights = jnp.exp(scores - jnp.max(scores, axis=-1, keepdims=True))
        totals = jnp.sum(weights, axis=-1, keepdims=True)
        mixed = jnp.dot(weights.astype(bf16), values, preferred_element_type=f32)
        attended[:, h * head_dim : (h + 1) * head_dim] = (mixed / totals).astype(bf16)
    at(17)
    out_relay.flush()
    out_relay.settle()

    n_dev = n_grp * n_seq
    out_width = attn_out.shape[1]
    streamed = out_width % LANES != 0
    ahead = AHEAD if streamed else 0
    out_loads = [
        pltpu.make_async_copy(out_all.at[i], out_v.at[i % AHEAD], out_sem.at[i % AHEAD])
        for i in range(n_dev if streamed else 0)
    ]
    for i in range(ahead):
        out_loads[i].start()
    stores = []
    for c in range(n_seq):
        for j in range(n_grp):
            i = c * n_grp + j
            if streamed:
                out_loads[i].wait()
            weight = out_v[i % AHEAD] if streamed else out_all[i]
            update = jnp.dot(attended[...], weight, preferred_element_type=f32)
            if streamed and i + AHEAD < n_dev:
                out_loads[i + AHEAD].start()
            columns = slice(j * out_width, (j + 1) * out_width)
            held = chunk(c)
            held[:, columns] = (held[:, columns].astype(f32) + update).astype(bf16)
        stores.append(
            pltpu.make_async_copy(chunk(c), result.at[:, chunk_columns(c)], result_sem.at[c])
        )
        stores[-1].start()
    for store in stores:
        store.wait()
    first.end()
    second.end()
    for move in table_moves:
        move.wait_send()
    for there, move in kv_moves:
        pl.when(there)(move.wait_send)
    relay.end()
    out_relay.end()


VMEM = pl.BlockSpec(memory_space=pltpu.VMEM)
SMEM = pl.BlockSpec(memory_space=pltpu.SMEM)
ANY = pl.BlockSpec(memory_space=pl.ANY)


def on_device(
    patches, piece_ids, vit_gain, vit_qkv, vit_out, merge_gain, merge_up, merge_down, dest,
    tokens, image_index, doc_lengths, attn_gain, attn_qkv, attn_out,
):
    rows, features = patches.shape
    n_seq, n_grp = lax.axis_size("seq"), lax.axis_size("grp")
    n_dev = n_seq * n_grp
    own = rows // 4
    capacity = own // (n_seq // 2)
    slots = n_seq * capacity
    reach = n_seq // 2
    line = n_seq // 2
    bf16, f32 = jnp.bfloat16, jnp.float32
    tok_rows = tokens.shape[0]
    query_width, out_width = attn_out.shape
    kv_width = attn_qkv.shape[1] - query_width
    down_width = merge_down.shape[1]
    dma = pltpu.SemaphoreType.DMA
    streamed = out_width % LANES != 0
    out_all_shape = (n_dev,) + attn_out.shape
    outputs = [jax.ShapeDtypeStruct(tokens.shape, bf16)]
    held = [pltpu.VMEM(out_all_shape, bf16)]
    if streamed:
        outputs.append(jax.ShapeDtypeStruct(out_all_shape, bf16))
        held = []
    results = pl.pallas_call(
        functools.partial(layer_kernel, n_grp, n_seq, capacity, reach),
        out_shape=tuple(outputs),
        in_specs=[VMEM] * 6 + [SMEM] * 2 + [ANY] * 7,
        out_specs=(ANY,) * len(outputs),
        scratch_shapes=held + [
            pltpu.VMEM(vit_qkv.shape, bf16),
            pltpu.VMEM(vit_out.shape, bf16),
            pltpu.VMEM(merge_up.shape, bf16),
            pltpu.VMEM(merge_down.shape, bf16),
            pltpu.VMEM((n_dev,) + attn_qkv.shape, bf16),
            pltpu.VMEM((features // LANES, rows, LANES), f32),
            pltpu.VMEM((n_seq, own, 4 * features + LANES), bf16),
            pltpu.VMEM((n_seq, n_seq * own, merge_up.shape[1]), bf16),
            pltpu.VMEM((n_seq, slots, down_width), bf16),
            pltpu.VMEM((n_seq, slots, down_width), bf16),
            pltpu.VMEM((tok_rows, query_width), bf16),
            pltpu.VMEM((reach + 1, tok_rows, kv_width), bf16),
            pltpu.VMEM((tok_rows, query_width), bf16),
            pltpu.VMEM((AHEAD, query_width if streamed else 16, out_width), bf16),
            dma((6,)), dma((n_seq,)), dma((n_seq,)), dma((AHEAD,)),
            dma((3, line)), dma((3, line)), dma((n_seq,)), dma((n_seq,)),
            dma((n_seq,)), dma((n_seq,)), dma((reach + 2,)), dma((reach + 1,)),
        ] + relay_scratch(n_dev) + relay_scratch(n_dev),
        compiler_params=pltpu.CompilerParams(
            collective_id=0, has_side_effects=True, vmem_limit_bytes=67043328
        ),
    )(
        patches, piece_ids, vit_gain, merge_gain, attn_gain, image_index, dest, doc_lengths,
        vit_qkv, vit_out, merge_up, merge_down, tokens, attn_qkv, attn_out,
    )
    return results[0]


def solution(mesh):
    placed = (
        P(("grp", "seq"), None),
        P(("grp", "seq"), None),
        P(),
        P(),
        P(),
        P(),
        P(None, "seq"),
        P(None, "seq"),
        P(("grp", "seq")),
        P(("grp", "seq"), None),
        P(("grp", "seq")),
        P("grp", None),
        P(),
        P(("grp", "seq"), None),
        P(None, ("grp", "seq")),
    )
    return jax.shard_map(
        on_device, mesh=mesh, in_specs=placed, out_specs=P(("grp", "seq"), None), check_vma=False
    )
```
